32 devices in a mesh: pool: 8 (over z, y), band: 4 (over x, core).
Axes of the slice: x: 2, y: 2, z: 4, core: 2. Of those that a mesh axis runs over, the one named last changes fastest.
Arguments:
- orbitals: bfloat16 [8, 4, 2, 46656], P('pool', 'band'), may hold values from -6 to 6
- occupation: int32 [8, 4], P('pool', 'band'), may hold values from 1 to 2
- kernel: float32 [46656], replicated, may hold values from 0.02 to 2
Outputs:
- exchanged: bfloat16 [8, 4, 2, 46656], P('pool', 'band')
- gram_matrix: float32 [8, 2, 4, 4], P('pool', None, None, 'band')
The draws below stay inside these ranges and needn't reach their ends.
All inputs are finite; a program needn't handle non-finite values.
Results may differ from the reference program's by a relative error of at most 0.013.
Values may be sent and summed in bfloat16 or wider, within the bound.
No kernel may reach another device: no remote copies, remote signals or barrier semaphores. Data moves between devices by JAX's collectives and lax.ppermute only.
A program may use at most 64 MiB of HBM per device.

```python
import math
import jax
import jax.numpy as jnp
from jax import lax

NG = 36
BAND_DEV = 1
GRID = 46656
NB = 4
K = 8
N_POOL = 8
N_BAND = 4


def place_ends(drawn, stream_key, low, largest):
    dims = drawn.shape
    spot = [jax.random.randint(jax.random.fold_in(stream_key, axis), (), 0, dims[axis]) for axis in range(len(dims))]
    drawn = drawn.at[tuple(spot)].set(low)
    longest = dims.index(max(dims))
    spot[longest] = (spot[longest] + 1) % dims[longest]
    return drawn.at[tuple(spot)].set(largest)


def block_scale(rng, shape, cuts, low, high):
    factor_of, own = 1.0, jax.random.fold_in(rng, 6)
    for dim, shards_of in cuts:
        draws = jnp.exp(jax.random.uniform(jax.random.fold_in(own, dim), (shards_of,), jnp.float32, low / len(cuts), high / len(cuts)))
        factor_of = factor_of * jnp.repeat(draws, shape[dim] // shards_of).reshape([-1 if axis == dim else 1 for axis in range(len(shape))])
    return factor_of


def gaussian(rng, extent, scale, most, cuts=(), kind=jnp.bfloat16):
    array = jax.random.normal(rng, extent, jnp.float32) * scale
    if len(cuts) > 0:
        array = block_scale(rng, extent, cuts, -0.22, 0.18) * array
    return jnp.clip(array, min=-most, max=most).astype(kind)


def setup_inputs(seed: int = 0) -> dict:
    keys = jax.random.split(jax.random.key(seed), 4)
    orbitals = gaussian(keys[0], (K, NB, 2, GRID), 1.0, 6.0, ((0, 8), (1, 4)))
    occupation = place_ends(jax.random.randint(keys[1], (K, NB), 1, 3), jax.random.fold_in(keys[1], 1), 1, 2).astype(jnp.int32)
    kernel = jnp.clip(jnp.exp(jax.random.uniform(keys[2], (GRID,), jnp.float32, math.log(0.02), math.log(2.0))), 0.02, 2.0)
    return dict(orbitals=orbitals, occupation=occupation, kernel=kernel)


def start_of(*values):
    return tuple((jnp.asarray(value, dtype=jnp.int32) for value in values))

def dft_matrix(direction):
    points = jnp.arange(NG, dtype=jnp.int32)
    phases = points[:, None] * points[None, :] % NG
    angles = 2.0 * math.pi / NG * phases.astype(jnp.float32)
    cosine = jnp.cos(angles)
    sine = direction * jnp.sin(angles)
    blocks = jnp.stack([jnp.stack([cosine, sine]), jnp.stack([-sine, cosine])])
    return jnp.transpose(blocks, (0, 2, 1, 3)).astype(jnp.bfloat16)

def transform(values, matrix, keep_float):
    count = values.shape[0]
    current = values.reshape(count, 2, NG, NG * NG)
    for axis_pass in range(3):
        product = jnp.einsum('uavb,pvbc->puca', matrix.astype(jnp.float32), current.astype(jnp.float32), precision=lax.Precision.HIGHEST)
        product = product.reshape(count, 2, NG, NG * NG)
        if axis_pass == 2 and keep_float:
            current = product
        else:
            current = product.astype(jnp.bfloat16)
    return current.reshape(count, 2, NG * NG * NG)

def add_block(accum_real, accum_imag, local_bands, visiting, visiting_occ, kernel, forward_matrix, inverse_matrix):
    c = local_bands[:, 0].astype(jnp.float32)
    d = local_bands[:, 1].astype(jnp.float32)
    for j in range(visiting.shape[0]):
        a = visiting[j, 0].astype(jnp.float32)
        b = visiting[j, 1].astype(jnp.float32)
        density = jnp.stack([a * c + b * d, a * d - b * c], axis=1).astype(jnp.bfloat16)
        spectrum = transform(density, forward_matrix, False)
        screened = (spectrum.astype(jnp.float32) * (kernel / GRID)).astype(jnp.bfloat16)
        potential = transform(screened, inverse_matrix, True)
        weight = -0.5 * visiting_occ[j].astype(jnp.float32)
        e = potential[:, 0]
        f = potential[:, 1]
        accum_real = accum_real + weight * (a * e - b * f)
        accum_imag = accum_imag + weight * (a * f + b * e)
    return (accum_real, accum_imag)

def contract(x, y):
    return jnp.einsum('ig,jg->ij', x.astype(jnp.float32), y.astype(jnp.float32), precision=lax.Precision.HIGHEST)

def gram_block(bra_rows, ket_rows):
    c = bra_rows[:, 0]
    d = bra_rows[:, 1]
    e = ket_rows[:, 0]
    f = ket_rows[:, 1]
    real_part = contract(c, e) + contract(d, f)
    imag_part = contract(c, f) - contract(d, e)
    return jnp.stack([real_part, imag_part])

def reference(orbitals, occupation, kernel):
    forward_matrix = dft_matrix(1.0)
    inverse_matrix = dft_matrix(-1.0)

    def per_group(pool_index, group_index):
        before = (pool_index + N_POOL - 1) % N_POOL
        prior = (group_index + N_BAND - 1) % N_BAND
        local_bands = lax.dynamic_slice(orbitals, start_of(pool_index, group_index * BAND_DEV, 0, 0), (1, BAND_DEV, 2, GRID))[0]
        first_block = lax.dynamic_slice(orbitals, start_of(before, group_index * BAND_DEV, 0, 0), (1, BAND_DEV, 2, GRID))[0]
        second_block = lax.dynamic_slice(orbitals, start_of(before, prior * BAND_DEV, 0, 0), (1, BAND_DEV, 2, GRID))[0]
        first_occ = lax.dynamic_slice(occupation, start_of(before, group_index * BAND_DEV), (1, BAND_DEV))[0]
        second_occ = lax.dynamic_slice(occupation, start_of(before, prior * BAND_DEV), (1, BAND_DEV))[0]
        zeros_grid = jnp.zeros((BAND_DEV, GRID), jnp.float32)
        accum_real, accum_imag = add_block(zeros_grid, zeros_grid, local_bands, first_block, first_occ, kernel, forward_matrix, inverse_matrix)
        accum_real, accum_imag = add_block(accum_real, accum_imag, local_bands, second_block, second_occ, kernel, forward_matrix, inverse_matrix)
        return jnp.stack([accum_real, accum_imag], axis=1).astype(jnp.bfloat16)
    groups = jnp.arange(N_BAND, dtype=jnp.int32)

    def per_pool(pool_index):
        return jax.vmap(lambda group_index: per_group(pool_index, group_index))(groups)
    exchanged = lax.map(per_pool, jnp.arange(N_POOL, dtype=jnp.int32)).reshape(N_POOL, BAND_DEV * N_BAND, 2, GRID)
    norm_factor = 1.0 / math.sqrt(GRID)

    def pool_gram(both):
        return gram_block(both[0], both[1]) * norm_factor
    gram_matrix = lax.map(pool_gram, (orbitals, exchanged))
    return (exchanged, gram_matrix)
```

```python
import math

import jax
import jax.numpy as jnp
import numpy as np
from jax import lax
from jax.experimental import pallas as pl
from jax.experimental.pallas import tpu as pltpu
from jax.sharding import PartitionSpec as P

LANES = 128
F32 = jnp.float32
BF16 = jnp.bfloat16
VMEM = pl.BlockSpec(memory_space=pltpu.VMEM)
SMEM = pl.BlockSpec(memory_space=pltpu.SMEM)


class Plan:
    def __init__(self, grid):
        ng = round(grid ** (1.0 / 3.0))
        self.grid = grid
        self.ng = ng
        self.split = max(b for b in range(1, ng + 1) if ng % b == 0 and b * ng <= LANES)
        self.coarse = ng // self.split
        self.width = self.split * ng
        self.rows = grid // self.width
        self.tiles = grid // LANES + 1
        self.tail = grid % LANES
        common = math.lcm(self.width, LANES)
        self.row_period = common // self.width
        self.tile_period = common // LANES
        self.padded_rows = (self.rows // self.row_period + 1) * self.row_period + 8
        self.padded_tiles = (self.tiles // self.tile_period + 1) * self.tile_period + 8


def roots(ng, phases):
    angles = 2.0 * np.pi / ng * (phases % ng)
    return np.cos(angles), np.sin(angles)


def constants(plan):
    ng, split, coarse, width = plan.ng, plan.split, plan.coarse, plan.width
    x, a = np.divmod(np.arange(plan.rows), coarse)
    b, z = np.divmod(np.arange(width), ng)
    cosine, sine = roots(ng, np.outer(x, x) + split * np.outer(a, a))
    left = np.concatenate([cosine, sine], axis=1)
    cosine, sine = roots(ng, coarse * np.outer(b, b) + np.outer(z, z))
    right = np.zeros((2, 2, LANES, 2, LANES))
    for way, sign in enumerate((1.0, -1.0)):
        right[way, 0, :width, 0, :width] = cosine
        right[way, 1, :width, 1, :width] = cosine
        right[way, 1, :width, 0, :width] = sign * sine
        right[way, 0, :width, 1, :width] = -sign * sine
    twiddle = np.zeros((2, plan.rows, LANES))
    twiddle[0, :, :width], twiddle[1, :, :width] = roots(ng, np.outer(a, b))
    return (
        jnp.asarray(left, BF16),
        jnp.asarray(right.reshape(2, 2 * LANES, 2 * LANES), BF16),
        jnp.asarray(twiddle, F32),
    )


def pack(plan):
    def body(orbital, occupation, out):
        last = plan.tiles - 1
        for q in range(last):
            out[2 * q : 2 * q + 2, :] = orbital[:, LANES * q : LANES * (q + 1)]
        if plan.tail:
            out[2 * last :, : plan.tail] = orbital[:, LANES * last :]
        fill = jnp.full((2, LANES - plan.tail), occupation[0], jnp.int32)
        out[2 * last :, plan.tail :] = fill.astype(F32).astype(BF16)

    return pl.pallas_call(
        body,
        out_shape=jax.ShapeDtypeStruct((2 * plan.tiles, LANES), BF16),
        in_specs=[VMEM, SMEM],
        out_specs=VMEM,
        name="pack",
    )


def to_matrix(plan, tiles, store):
    for j in range(plan.row_period):
        q, shift = divmod(plan.width * j, LANES)
        count = -(-(plan.rows - j) // plan.row_period)
        stride = 2 * plan.tile_period
        for part in range(2):
            block = tiles[pl.ds(2 * q + part, count, stride=stride), :]
            if shift + plan.width > LANES:
                after = tiles[pl.ds(2 * q + 2 + part, count, stride=stride), :]
                lane = lax.broadcasted_iota(jnp.int32, block.shape, 1)
                block = jnp.where(lane >= shift, block, after)
            if shift:
                block = pltpu.roll(block, LANES - shift, axis=1)
            store(part, j, count, block)


def from_matrix(plan, matrix, tiles):
    width = plan.width
    for i in range(plan.tile_period):
        row, offset = divmod(LANES * i, width)
        count = -(-(plan.tiles - i) // plan.tile_period)
        for part in range(2):
            block = None
            start = -offset
            while start < LANES:
                rows = matrix[part, pl.ds(row, count, stride=plan.row_period), :]
                if start % LANES:
                    rows = pltpu.roll(rows, start % LANES, axis=1)
                if block is None:
                    block = rows
                else:
                    lane = lax.broadcasted_iota(jnp.int32, rows.shape, 1)
                    block = jnp.where(lane < start, block, rows)
                start += width
                row += 1
            row -= -(-(LANES + offset) // width)
            tiles[pl.ds(2 * i + part, count, stride=2 * plan.tile_period), :] = block


def exchange(plan, own, tiles, near, fourier, kernel, left, right, twiddle):
    rows = plan.rows

    def keep(part, first, count, block):
        near[part, pl.ds(first, count, stride=plan.row_period), :] = block

    to_matrix(plan, tiles, keep)
    c = own[0, :rows, :]
    d = own[1, :rows, :]
    a = near[0, :rows, :]
    b = near[1, :rows, :]

    def put(real, imag, sign):
        real = real.astype(BF16)
        imag = imag.astype(BF16)
        fourier[:rows, :LANES] = real
        fourier[:rows, LANES:] = imag
        fourier[rows:, :LANES] = imag if sign > 0 else -imag
        fourier[rows:, LANES:] = -real if sign > 0 else real

    def dot(x, y):
        return jnp.dot(x, y, preferred_element_type=F32)

    put(a * c + b * d, a * d - b * c, 1)
    half = dot(left[...], fourier[...])
    real, imag = half[:, :LANES], half[:, LANES:]
    cosine = twiddle[0]
    sine = twiddle[1]
    turned = jnp.concatenate(
        [real * cosine + imag * sine, imag * cosine - real * sine], axis=1
    ).astype(BF16)
    spectrum = dot(turned, right[0])
    factor = kernel[...]
    screened = jnp.concatenate(
        [spectrum[:, :LANES] * factor, spectrum[:, LANES:] * factor], axis=1
    ).astype(BF16)
    half = dot(screened, right[1])
    real, imag = half[:, :LANES], half[:, LANES:]
    put(real * cosine - imag * sine, imag * cosine + real * sine, -1)
    potential = dot(left[...], fourier[...])
    e = potential[:, :LANES]
    f = potential[:, LANES:]
    last = 2 * plan.tiles - 2
    weight = -0.5 * tiles[last : last + 1, plan.tail : plan.tail + 1]
    a = near[0, :rows, :]
    b = near[1, :rows, :]
    return weight * (a * e - b * f), weight * (a * f + b * e)


def first_pair(plan, others):
    def body(*refs):
        own_in, near_in, kernel, left, right, twiddle = refs[:6]
        band_in = refs[6 : 6 + others]
        own, accum, bands, tiles, near, fourier = refs[6 + others :]
        size = 2 * plan.tiles

        def keep_own(part, first, count, block):
            own[part, pl.ds(first, count, stride=plan.row_period), :] = block

        tiles[:size, :] = own_in[...].astype(F32)
        to_matrix(plan, tiles, keep_own)
        tiles[:size, :] = near_in[...].astype(F32)
        real, imag = exchange(plan, own, tiles, near, fourier, kernel, left, right, twiddle)
        accum[0] = real
        accum[1] = imag
        for index in range(others):

            def keep_band(part, first, count, block):
                bands[index, part, pl.ds(first, count, stride=plan.row_period), :] = block

            tiles[:size, :] = band_in[index][...].astype(F32)
            to_matrix(plan, tiles, keep_band)

    rows = plan.rows
    return pl.pallas_call(
        body,
        out_shape=[
            jax.ShapeDtypeStruct((2, rows, LANES), F32),
            jax.ShapeDtypeStruct((2, rows, LANES), F32),
            jax.ShapeDtypeStruct((others, 2, rows, LANES), F32),
        ],
        in_specs=[VMEM] * (6 + others),
        out_specs=[VMEM] * 3,
        scratch_shapes=[
            pltpu.VMEM((2 * plan.padded_tiles, LANES), F32),
            pltpu.VMEM((2, plan.padded_rows, LANES), F32),
            pltpu.VMEM((2 * rows, 2 * LANES), BF16),
        ],
        name="first_pair",
    )


def second_pair(plan, others):
    count = others + 1

    def body(place, own, accum, bands, far_in, near_in, kernel, left, right, twiddle, out, gram, *scratch):
        tiles, near, fourier, total = scratch
        size = 2 * plan.tiles
        odd = place[0] % 2 == 1
        tiles[:size, :] = jnp.where(odd, near_in[...].astype(F32), far_in[...].astype(F32))
        real, imag = exchange(plan, own, tiles, near, fourier, kernel, left, right, twiddle)
        e = (accum[0] + real).astype(BF16).astype(F32)
        f = (accum[1] + imag).astype(BF16).astype(F32)
        total[0, : plan.rows, :] = e
        total[1, : plan.rows, :] = f
        lane = lax.broadcasted_iota(jnp.int32, (1, count), 1)
        sums = [jnp.zeros((1, count), F32)] * 2
        norm = 1.0 / math.sqrt(plan.grid)
        for index in range(count):
            c = own[0] if index == 0 else bands[index - 1, 0]
            d = own[1] if index == 0 else bands[index - 1, 1]
            parts = (c * e + d * f, c * f - d * e)
            for part in range(2):
                value = jnp.sum(jnp.sum(parts[part], axis=0, keepdims=True), axis=1, keepdims=True)
                sums[part] = jnp.where(lane == place[index], value * norm, sums[part])
        for part in range(2):
            gram[part] = sums[part]
        from_matrix(plan, total, tiles)
        last = plan.tiles - 1
        for q in range(last):
            out[:, LANES * q : LANES * (q + 1)] = tiles[2 * q : 2 * q + 2, :].astype(BF16)
        if plan.tail:
            out[:, LANES * last :] = tiles[2 * last : 2 * last + 2, : plan.tail].astype(BF16)

    rows = plan.rows
    return pl.pallas_call(
        body,
        out_shape=[
            jax.ShapeDtypeStruct((2, plan.grid), BF16),
            jax.ShapeDtypeStruct((2, 1, count), F32),
        ],
        in_specs=[SMEM] + [VMEM] * 9,
        out_specs=[VMEM] * 2,
        scratch_shapes=[
            pltpu.VMEM((2 * plan.padded_tiles, LANES), F32),
            pltpu.VMEM((2, plan.padded_rows, LANES), F32),
            pltpu.VMEM((2 * rows, 2 * LANES), BF16),
            pltpu.VMEM((2, plan.padded_rows, LANES), F32),
        ],
        name="second_pair",
    )


def shards(orbitals, occupation, kernel):
    plan = Plan(orbitals.shape[3])
    pools = lax.axis_size("pool")
    groups = lax.axis_size("band")

    def move(array, target):
        pairs = [
            (p * groups + g, q * groups + h)
            for p in range(pools)
            for g in range(groups)
            for q, h in [target(p, g)]
        ]
        return lax.ppermute(array, ("pool", "band"), pairs)

    own = pack(plan)(orbitals[0, 0], occupation[0])
    near = move(own, lambda p, g: ((p + 1) % pools, g))
    far = move(
        own,
        lambda p, g: ((p + 1) % pools, (g + 1) % groups) if g % 2 else (p, g + 1),
    )
    partner = lambda p, g: (p, g ^ 1)
    bands = [move(own, partner)]
    for step in range(1, groups // 2):
        shifted = move(own, lambda p, g: (p, (g + 2 * step) % groups))
        bands += [shifted, move(shifted, partner)]
    swapped = move(near, partner)
    here = lax.axis_index("band")
    places = [here, here ^ 1]
    for step in range(1, groups // 2):
        places += [(here - 2 * step) % groups, ((here ^ 1) - 2 * step) % groups]
    place = jnp.stack(places).astype(jnp.int32)

    factor = kernel.reshape(plan.ng, plan.split, plan.coarse, plan.ng).transpose(0, 2, 1, 3)
    factor = factor.reshape(plan.rows, plan.width) * (1.0 / plan.grid)
    factor = jnp.pad(factor, ((0, 0), (0, LANES - plan.width)))
    left, right, twiddle = constants(plan)
    others = groups - 1
    mine, accum, stack = first_pair(plan, others)(own, near, factor, left, right, twiddle, *bands)
    exchanged, gram = second_pair(plan, others)(
        place, mine, accum, stack, far, swapped, factor, left, right, twiddle
    )
    return exchanged[None, None], jnp.swapaxes(gram, 1, 2)[None]


def solution(mesh):
    return jax.shard_map(
        shards,
        mesh=mesh,
        in_specs=(P("pool", "band", None, None), P("pool", "band"), P()),
        out_specs=(P("pool", "band", None, None), P("pool", None, None, "band")),
        check_vma=False,
    )
```

```python
import math

import jax
import jax.numpy as jnp
import numpy as np
from jax import lax
from jax.experimental import pallas as pl
from jax.experimental.pallas import tpu as pltpu
from jax.sharding import PartitionSpec as P


LANES = 128
F32 = jnp.float32
BF16 = jnp.bfloat16
VMEM = pl.BlockSpec(memory_space=pltpu.VMEM)
SMEM = pl.BlockSpec(memory_space=pltpu.SMEM)
HBM = pl.BlockSpec(memory_space=pl.ANY)


class Plan:
    def __init__(self, grid):
        ng = round(grid ** (1.0 / 3.0))
        self.grid = grid
        self.ng = ng
        self.split = max(b for b in range(1, ng + 1) if ng % b == 0 and b * ng <= LANES)
        self.coarse = ng // self.split
        self.width = self.split * ng
        self.rows = grid // self.width
        self.tiles = grid // LANES + 1
        self.tail = grid % LANES
        common = math.lcm(self.width, LANES)
        self.row_period = common // self.width
        self.tile_period = common // LANES
        self.blocks = -(-self.rows // self.row_period)
        self.kept = self.blocks * self.row_period
        self.padded_tiles = (self.blocks * self.tile_period + 15) // 8 * 8


def roots(ng, phases):
    angles = 2.0 * np.pi / ng * (phases % ng)
    return np.cos(angles), np.sin(angles)


def constants(plan):
    ng, split, coarse, width = plan.ng, plan.split, plan.coarse, plan.width
    j, block = np.divmod(np.arange(plan.kept), plan.blocks)
    row = block * plan.row_period + j
    real_row = row < plan.rows
    x, a = np.divmod(row, coarse)
    b, z = np.divmod(np.arange(width), ng)
    mask = np.outer(real_row, real_row)
    cosine, sine = roots(ng, np.outer(x, x) + split * np.outer(a, a))
    left = np.concatenate([cosine * mask, sine * mask], axis=1)
    cosine, sine = roots(ng, coarse * np.outer(b, b) + np.outer(z, z))
    right = np.zeros((2, 2, LANES, 2, LANES))
    for way, sign in enumerate((1.0, -1.0)):
        right[way, 0, :width, 0, :width] = cosine
        right[way, 1, :width, 1, :width] = cosine
        right[way, 1, :width, 0, :width] = sign * sine
        right[way, 0, :width, 1, :width] = -sign * sine
    twiddle = np.zeros((2, plan.kept, LANES))
    twiddle[0, :, :width], twiddle[1, :, :width] = roots(ng, np.outer(a, b))
    return (
        jnp.asarray(left, BF16),
        jnp.asarray(right.reshape(2, 2 * LANES, 2 * LANES), BF16),
        jnp.asarray(twiddle, F32),
    )


def pack(plan):
    def body(orbital, occupation, out):
        last = plan.tiles - 1
        for q in range(last):
            out[2 * q : 2 * q + 2, :] = orbital[:, LANES * q : LANES * (q + 1)]
        if plan.tail:
            out[2 * last :, : plan.tail] = orbital[:, LANES * last :]
        fill = jnp.full((2, LANES - plan.tail), occupation[0], jnp.int32)
        out[2 * last :, plan.tail :] = fill.astype(F32).astype(BF16)

    return pl.pallas_call(
        body,
        out_shape=jax.ShapeDtypeStruct((2 * plan.tiles, LANES), BF16),
        in_specs=[VMEM, SMEM],
        out_specs=VMEM,
        compiler_params=pltpu.CompilerParams(vmem_limit_bytes=4 * 1024 * 1024),
        name="pack",
    )


def shifted_rows(plan, tiles, first, step, j):
    q, shift = divmod(plan.width * j, LANES)
    stride = step * plan.tile_period
    rows = tiles[pl.ds(step * q + first, plan.blocks, stride=stride), :]
    if shift + plan.width > LANES:
        after = tiles[pl.ds(step * (q + 1) + first, plan.blocks, stride=stride), :]
        lane = lax.broadcasted_iota(jnp.int32, rows.shape, 1)
        rows = jnp.where(lane >= shift, rows, after)
    return pltpu.roll(rows, LANES - shift, axis=1) if shift else rows


def to_matrix(plan, packed, tiles, matrix):
    size = 2 * plan.tiles
    tiles[:size, :] = packed.astype(F32)
    tiles[size:, :] = jnp.zeros((2 * plan.padded_tiles - size, LANES), F32)
    for j in range(plan.row_period):
        for part in range(2):
            rows = shifted_rows(plan, tiles, part, 2, j)
            matrix[part, plan.blocks * j : plan.blocks * (j + 1), :] = rows


def from_matrix(plan, matrix, tiles):
    width, blocks = plan.width, plan.blocks
    for i in range(plan.tile_period):
        for part in range(2):
            row, offset = divmod(LANES * i, width)
            flat = None
            start = -offset
            while start < LANES:
                turn, j = divmod(row, plan.row_period)
                rows = matrix[part, blocks * j + turn : blocks * (j + 1) + turn, :]
                if start % LANES:
                    rows = pltpu.roll(rows, start % LANES, axis=1)
                if flat is None:
                    flat = rows
                else:
                    lane = lax.broadcasted_iota(jnp.int32, rows.shape, 1)
                    flat = jnp.where(lane < start, flat, rows)
                start += width
                row += 1
            tiles[blocks * (2 * i + part) : blocks * (2 * i + part + 1), :] = flat


def prepare(plan):
    split, coarse, ng = plan.split, plan.coarse, plan.ng

    def body(own_in, kernel_in, left, right, twiddle, own, factor, left_out, right_out, twiddle_out, tiles, plain, ordered, arrived):
        copies = [
            pltpu.make_async_copy(source, target, arrived.at[index])
            for index, (source, target) in enumerate(
                ((left, left_out), (right, right_out), (twiddle, twiddle_out))
            )
        ]
        for copy in copies:
            copy.start()
        to_matrix(plan, own_in[...], tiles, own)
        for j in range(plan.row_period):
            rows = shifted_rows(plan, kernel_in, 0, 1, j)
            plain[pl.ds(j, plan.blocks, stride=plan.row_period), :] = rows * (1.0 / plan.grid)
        lane = lax.broadcasted_iota(jnp.int32, (ng, LANES), 1)
        for a in range(coarse):
            rows = None
            for b in range(split):
                row, column = divmod(a + coarse * b, split)
                piece = plain[pl.ds(row, ng, stride=coarse), :]
                shift = (ng * (b - column)) % LANES
                if shift:
                    piece = pltpu.roll(piece, shift, axis=1)
                rows = piece if rows is None else jnp.where(lane < ng * b, rows, piece)
            ordered[pl.ds(a, ng, stride=coarse), :] = rows
        ordered[plan.rows :, :] = jnp.zeros((plan.kept - plan.rows, LANES), F32)
        for j in range(plan.row_period):
            rows = ordered[pl.ds(j, plan.blocks, stride=plan.row_period), :]
            factor[plan.blocks * j : plan.blocks * (j + 1), :] = rows
        for copy in copies:
            copy.wait()

    return pl.pallas_call(
        body,
        out_shape=[
            jax.ShapeDtypeStruct((2, plan.kept, LANES), F32),
            jax.ShapeDtypeStruct((plan.kept, LANES), F32),
            jax.ShapeDtypeStruct((plan.kept, 2 * plan.kept), BF16),
            jax.ShapeDtypeStruct((2, 2 * LANES, 2 * LANES), BF16),
            jax.ShapeDtypeStruct((2, plan.kept, LANES), F32),
        ],
        in_specs=[VMEM] * 2 + [HBM] * 3,
        out_specs=[VMEM] * 5,
        scratch_shapes=[
            pltpu.VMEM((2 * plan.padded_tiles, LANES), F32),
            pltpu.VMEM((plan.kept, LANES), F32),
            pltpu.VMEM((plan.kept, LANES), F32),
            pltpu.SemaphoreType.DMA((3,)),
        ],
        compiler_params=pltpu.CompilerParams(vmem_limit_bytes=4 * 1024 * 1024),
        name="prepare",
    )


def exchange(plan, own, packed, tiles, near, fourier, kernel, left, right, twiddle):
    rows = plan.kept
    to_matrix(plan, packed, tiles, near)
    c = own[0]
    d = own[1]
    a = near[0]
    b = near[1]

    def put(real, imag, sign):
        real = real.astype(BF16)
        imag = imag.astype(BF16)
        fourier[:rows, :LANES] = real
        fourier[:rows, LANES:] = imag
        fourier[rows:, :LANES] = imag if sign > 0 else -imag
        fourier[rows:, LANES:] = -real if sign > 0 else real

    def dot(x, y):
        return jnp.dot(x, y, preferred_element_type=F32)

    put(a * c + b * d, a * d - b * c, 1)
    half = dot(left[...], fourier[...])
    real, imag = half[:, :LANES], half[:, LANES:]
    cosine = twiddle[0]
    sine = twiddle[1]
    turned = jnp.concatenate(
        [real * cosine + imag * sine, imag * cosine - real * sine], axis=1
    ).astype(BF16)
    spectrum = dot(turned, right[0])
    factor = kernel[...]
    screened = jnp.concatenate(
        [spectrum[:, :LANES] * factor, spectrum[:, LANES:] * factor], axis=1
    ).astype(BF16)
    half = dot(screened, right[1])
    real, imag = half[:, :LANES], half[:, LANES:]
    put(real * cosine - imag * sine, imag * cosine + real * sine, -1)
    potential = dot(left[...], fourier[...])
    e = potential[:, :LANES]
    f = potential[:, LANES:]
    last = 2 * plan.tiles - 2
    weight = -0.5 * tiles[last : last + 1, plan.tail : plan.tail + 1]
    a = near[0]
    b = near[1]
    return weight * (a * e - b * f), weight * (a * f + b * e)


def scratch_of(plan):
    return [
        pltpu.VMEM((2 * plan.padded_tiles, LANES), F32),
        pltpu.VMEM((2, plan.kept, LANES), F32),
        pltpu.VMEM((2 * plan.kept, 2 * LANES), BF16),
    ]


def first_pair(plan):
    def body(own, near_in, kernel, left, right, twiddle, pair_in, accum, pair, tiles, near, fourier):
        real, imag = exchange(plan, own, near_in[...], tiles, near, fourier, kernel, left, right, twiddle)
        accum[0] = real
        accum[1] = imag
        to_matrix(plan, pair_in[...], tiles, pair)

    matrix = jax.ShapeDtypeStruct((2, plan.kept, LANES), F32)
    return pl.pallas_call(
        body,
        out_shape=[matrix, matrix],
        in_specs=[VMEM] * 7,
        out_specs=[VMEM] * 2,
        scratch_shapes=scratch_of(plan),
        compiler_params=pltpu.CompilerParams(vmem_limit_bytes=16 * 1024 * 1024),
        name="first_pair",
    )


def second_pair(plan):
    def body(place, own, accum, far_in, near_in, kernel, left, right, twiddle, total, tiles, near, fourier):
        packed = jnp.where(place[0] % 2 == 1, near_in[...], far_in[...])
        real, imag = exchange(plan, own, packed, tiles, near, fourier, kernel, left, right, twiddle)
        total[0] = (accum[0] + real).astype(BF16).astype(F32)
        total[1] = (accum[1] + imag).astype(BF16).astype(F32)

    return pl.pallas_call(
        body,
        out_shape=jax.ShapeDtypeStruct((2, plan.kept, LANES), F32),
        in_specs=[SMEM] + [VMEM] * 8,
        out_specs=VMEM,
        scratch_shapes=scratch_of(plan),
        compiler_params=pltpu.CompilerParams(vmem_limit_bytes=16 * 1024 * 1024),
        name="second_pair",
    )


def finish(plan, others):
    count = others + 1

    def body(*refs):
        place, total, own, pair = refs[:4]
        bands = refs[4 : 3 + others]
        out, gram, tiles, matrix, flat, sent = refs[3 + others :]
        from_matrix(plan, total, tiles)
        for q in range(plan.tiles):
            turn, i = divmod(q, plan.tile_period)
            pair_rows = tiles[pl.ds(2 * plan.blocks * i + turn, 2, stride=plan.blocks), :].astype(BF16)
            used = min(LANES, plan.grid - LANES * q)
            if used:
                flat[:, LANES * q : LANES * q + used] = pair_rows[:, :used]
        copy = pltpu.make_async_copy(flat, out, sent)
        copy.start()
        lane = lax.broadcasted_iota(jnp.int32, (1, count), 1)
        sums = [jnp.zeros((1, count), F32)] * 2
        norm = 1.0 / math.sqrt(plan.grid)
        e = total[0]
        f = total[1]
        for index in range(count):
            if index < 2:
                band = (own, pair)[index]
                c, d = band[0], band[1]
            else:
                to_matrix(plan, bands[index - 2][...], tiles, matrix)
                c, d = matrix[0], matrix[1]
            parts = (c * e + d * f, c * f - d * e)
            for part in range(2):
                value = jnp.sum(jnp.sum(parts[part], axis=0, keepdims=True), axis=1, keepdims=True)
                sums[part] = jnp.where(lane == place[index], value * norm, sums[part])
        for part in range(2):
            gram[part] = sums[part]
        copy.wait()

    return pl.pallas_call(
        body,
        out_shape=[
            jax.ShapeDtypeStruct((2, plan.grid), BF16),
            jax.ShapeDtypeStruct((2, 1, count), F32),
        ],
        in_specs=[SMEM] + [VMEM] * (2 + others),
        out_specs=[HBM, VMEM],
        scratch_shapes=[
            pltpu.VMEM((2 * plan.padded_tiles, LANES), F32),
            pltpu.VMEM((2, plan.kept, LANES), F32),
            pltpu.VMEM((2, plan.grid), BF16),
            pltpu.SemaphoreType.DMA,
        ],
        compiler_params=pltpu.CompilerParams(vmem_limit_bytes=16 * 1024 * 1024),
        name="finish",
    )


def shards(orbitals, occupation, kernel):
    plan = Plan(orbitals.shape[3])
    pools = lax.axis_size("pool")
    groups = lax.axis_size("band")
    others = groups - 1

    def move(array, target):
        pairs = [
            (p * groups + g, q * groups + h)
            for p in range(pools)
            for g in range(groups)
            for q, h in [target(p, g)]
        ]
        return lax.ppermute(array, ("pool", "band"), pairs)

    here = lax.axis_index("band")
    places = [here, here ^ 1]
    for step in range(1, groups // 2):
        places += [(here - 2 * step) % groups, ((here ^ 1) - 2 * step) % groups]
    place = jnp.stack(places).astype(jnp.int32)
    own = pack(plan)(orbitals[0, 0], occupation[0])
    near = move(own, lambda p, g: ((p + 1) % pools, g))
    far = move(own, lambda p, g: ((p + 1) % pools, (g + 1) % groups) if g % 2 else (p, g + 1))
    partner = lambda p, g: (p, g ^ 1)
    bands = [move(own, partner)]
    for step in range(1, groups // 2):
        shifted = move(own, lambda p, g: (p, (g + 2 * step) % groups))
        bands += [shifted, move(shifted, partner)]
    swapped = move(near, partner)
    padded = jnp.pad(kernel, (0, plan.padded_tiles * LANES - plan.grid))
    mine, factor, left, right, twiddle = prepare(plan)(
        own, padded.reshape(-1, LANES), *constants(plan)
    )
    accum, pair = first_pair(plan)(mine, near, factor, left, right, twiddle, bands[0])
    total = second_pair(plan)(place, mine, accum, far, swapped, factor, left, right, twiddle)
    exchanged, gram = finish(plan, others)(place, total, mine, pair, *bands[1:])
    return exchanged[None, None], jnp.swapaxes(gram, 1, 2)[None]


def solution(mesh):
    return jax.shard_map(
        shards,
        mesh=mesh,
        in_specs=(P("pool", "band", None, None), P("pool", "band"), P()),
        out_specs=(P("pool", "band", None, None), P("pool", None, None, "band")),
        check_vma=False,
    )
```

```python
import math

import jax
import jax.numpy as jnp
import numpy as np
from jax import lax
from jax.experimental import pallas as pl
from jax.experimental.pallas import tpu as pltpu
from jax.sharding import PartitionSpec as P


LANES = 128
PARTS = 2
F32 = jnp.float32
BF16 = jnp.bfloat16
VMEM = pl.BlockSpec(memory_space=pltpu.VMEM)
SMEM = pl.BlockSpec(memory_space=pltpu.SMEM)
ANYWHERE = pl.BlockSpec(memory_space=pl.ANY)


class Plan:
    def __init__(self, grid):
        ng = round(grid ** (1.0 / 3.0))
        self.grid = grid
        self.ng = ng
        self.split = max(b for b in range(1, ng + 1) if ng % b == 0 and b * ng <= LANES)
        self.coarse = ng // self.split
        self.width = self.split * ng
        self.rows = grid // self.width
        self.tiles = grid // LANES + 1
        self.tail = grid % LANES
        common = math.lcm(self.width, LANES)
        self.row_period = common // self.width
        self.tile_period = common // LANES
        self.blocks = -(-self.rows // self.row_period)
        self.kept = self.blocks * self.row_period
        self.padded_tiles = (self.blocks * self.tile_period + 15) // 8 * 8


def roots(ng, phases):
    angles = 2.0 * np.pi / ng * (phases % ng)
    return np.cos(angles), np.sin(angles)


def constants(plan):
    ng, split, coarse, width = plan.ng, plan.split, plan.coarse, plan.width
    j, block = np.divmod(np.arange(plan.kept), plan.blocks)
    row = block * plan.row_period + j
    real_row = row < plan.rows
    x, a = np.divmod(row, coarse)
    b, z = np.divmod(np.arange(width), ng)
    mask = np.outer(real_row, real_row)
    cosine, sine = roots(ng, np.outer(x, x) + split * np.outer(a, a))
    left = np.concatenate([cosine * mask, sine * mask], axis=1)
    cosine, sine = roots(ng, coarse * np.outer(b, b) + np.outer(z, z))
    right = np.zeros((2, 2, LANES, 2, LANES))
    for way, sign in enumerate((1.0, -1.0)):
        right[way, 0, :width, 0, :width] = cosine
        right[way, 1, :width, 1, :width] = cosine
        right[way, 1, :width, 0, :width] = sign * sine
        right[way, 0, :width, 1, :width] = -sign * sine
    twiddle = np.zeros((2, plan.kept, LANES))
    twiddle[0, :, :width], twiddle[1, :, :width] = roots(ng, np.outer(a, b))
    return (
        jnp.asarray(left, BF16),
        jnp.asarray(right.reshape(2, 2 * LANES, 2 * LANES), BF16),
        jnp.asarray(twiddle, F32),
    )


def pack(plan):
    def body(orbital, occupation, out):
        last = plan.tiles - 1
        for q in range(last):
            out[2 * q : 2 * q + 2, :] = orbital[:, LANES * q : LANES * (q + 1)]
        if plan.tail:
            out[2 * last :, : plan.tail] = orbital[:, LANES * last :]
        fill = jnp.full((2, LANES - plan.tail), occupation[0], jnp.int32)
        out[2 * last :, plan.tail :] = fill.astype(F32).astype(BF16)

    return pl.pallas_call(
        body,
        out_shape=jax.ShapeDtypeStruct((2 * plan.tiles, LANES), BF16),
        in_specs=[VMEM, SMEM],
        out_specs=VMEM,
        compiler_params=pltpu.CompilerParams(vmem_limit_bytes=4 * 1024 * 1024),
        name="pack",
    )


def shifted_rows(plan, tiles, first, step, j):
    q, shift = divmod(plan.width * j, LANES)
    stride = step * plan.tile_period
    rows = tiles[pl.ds(step * q + first, plan.blocks, stride=stride), :]
    if shift + plan.width > LANES:
        after = tiles[pl.ds(step * (q + 1) + first, plan.blocks, stride=stride), :]
        lane = lax.broadcasted_iota(jnp.int32, rows.shape, 1)
        rows = jnp.where(lane >= shift, rows, after)
    return pltpu.roll(rows, LANES - shift, axis=1) if shift else rows


def to_matrix(plan, packed, tiles, matrix):
    size = 2 * plan.tiles
    tiles[:size, :] = packed.astype(F32)
    tiles[size:, :] = jnp.zeros((2 * plan.padded_tiles - size, LANES), F32)
    for j in range(plan.row_period):
        for part in range(2):
            rows = shifted_rows(plan, tiles, part, 2, j)
            matrix[part, plan.blocks * j : plan.blocks * (j + 1), :] = rows


def from_matrix(plan, matrix, tiles):
    width, blocks = plan.width, plan.blocks
    for i in range(plan.tile_period):
        for part in range(2):
            row, offset = divmod(LANES * i, width)
            flat = None
            start = -offset
            while start < LANES:
                turn, j = divmod(row, plan.row_period)
                rows = matrix[part, blocks * j + turn : blocks * (j + 1) + turn, :]
                if start % LANES:
                    rows = pltpu.roll(rows, start % LANES, axis=1)
                if flat is None:
                    flat = rows
                else:
                    lane = lax.broadcasted_iota(jnp.int32, rows.shape, 1)
                    flat = jnp.where(lane < start, flat, rows)
                start += width
                row += 1
            tiles[blocks * (2 * i + part) : blocks * (2 * i + part + 1), :] = flat


def prepare(plan):
    split, coarse, ng = plan.split, plan.coarse, plan.ng

    def body(own_in, kernel_in, left, right, twiddle, own, factor, tiles, plain, ordered):
        del left, right, twiddle
        to_matrix(plan, own_in[...], tiles, own)
        eight = 8 * LANES
        for q in range(0, plan.grid // eight):
            tiles[8 * q : 8 * q + 8, :] = kernel_in[eight * q : eight * (q + 1)].reshape(8, LANES)
        for q in range(plan.grid // eight * 8, plan.grid // LANES):
            tiles[q : q + 1, :] = kernel_in[LANES * q : LANES * (q + 1)].reshape(1, LANES)
        if plan.tail:
            q = plan.grid // LANES
            tiles[q : q + 1, : plan.tail] = kernel_in[LANES * q :].reshape(1, plan.tail)
        for j in range(plan.row_period):
            rows = shifted_rows(plan, tiles, 0, 1, j)
            plain[pl.ds(j, plan.blocks, stride=plan.row_period), :] = rows * (1.0 / plan.grid)
        lane = lax.broadcasted_iota(jnp.int32, (ng, LANES), 1)
        for a in range(coarse):
            rows = None
            for b in range(split):
                row, column = divmod(a + coarse * b, split)
                piece = plain[pl.ds(row, ng, stride=coarse), :]
                shift = (ng * (b - column)) % LANES
                if shift:
                    piece = pltpu.roll(piece, shift, axis=1)
                rows = piece if rows is None else jnp.where(lane < ng * b, rows, piece)
            ordered[pl.ds(a, ng, stride=coarse), :] = rows
        ordered[plan.rows :, :] = jnp.zeros((plan.kept - plan.rows, LANES), F32)
        for j in range(plan.row_period):
            rows = ordered[pl.ds(j, plan.blocks, stride=plan.row_period), :]
            factor[plan.blocks * j : plan.blocks * (j + 1), :] = rows

    return pl.pallas_call(
        body,
        out_shape=[
            jax.ShapeDtypeStruct((2, plan.kept, LANES), F32),
            jax.ShapeDtypeStruct((plan.kept, LANES), F32),
        ],
        in_specs=[VMEM] * 2 + [ANYWHERE] * 3,
        out_specs=[VMEM] * 2,
        scratch_shapes=[
            pltpu.VMEM((2 * plan.padded_tiles, LANES), F32),
            pltpu.VMEM((plan.kept, LANES), F32),
            pltpu.VMEM((plan.kept, LANES), F32),
        ],
        compiler_params=pltpu.CompilerParams(vmem_limit_bytes=4 * 1024 * 1024),
        name="prepare",
    )


def exchange(plan, own, packed, tiles, near, fourier, kernel, left, right, twiddle):
    rows = plan.kept
    to_matrix(plan, packed, tiles, near)
    c = own[0]
    d = own[1]
    a = near[0]
    b = near[1]

    step = rows // PARTS
    parts = [slice(step * index, step * (index + 1)) for index in range(PARTS)]

    def put(part, real, imag, sign):
        real = real.astype(BF16)
        imag = imag.astype(BF16)
        below = slice(rows + part.start, rows + part.stop)
        fourier[part, :LANES] = real
        fourier[part, LANES:] = imag
        fourier[below, :LANES] = imag if sign > 0 else -imag
        fourier[below, LANES:] = -real if sign > 0 else real

    def dot(x, y):
        return jnp.dot(x, y, preferred_element_type=F32)

    def split(value):
        return value[:, :LANES], value[:, LANES:]

    for part in parts:
        a, b, c, d = near[0, part, :], near[1, part, :], own[0, part, :], own[1, part, :]
        put(part, a * c + b * d, a * d - b * c, 1)
    halves = [dot(left[part, :], fourier[...]) for part in parts]
    for index, part in enumerate(parts):
        real, imag = split(halves[index])
        cosine, sine = twiddle[0, part, :], twiddle[1, part, :]
        halves[index] = jnp.concatenate(
            [real * cosine + imag * sine, imag * cosine - real * sine], axis=1
        ).astype(BF16)
    halves = [dot(value, right[0]) for value in halves]
    for index, part in enumerate(parts):
        real, imag = split(halves[index])
        factor = kernel[part, :]
        halves[index] = jnp.concatenate([real * factor, imag * factor], axis=1).astype(BF16)
    halves = [dot(value, right[1]) for value in halves]
    for index, part in enumerate(parts):
        real, imag = split(halves[index])
        cosine, sine = twiddle[0, part, :], twiddle[1, part, :]
        put(part, real * cosine - imag * sine, imag * cosine + real * sine, -1)
    potential = [dot(left[part, :], fourier[...]) for part in parts]
    results = []
    last = 2 * plan.tiles - 2
    weight = -0.5 * tiles[last : last + 1, plan.tail : plan.tail + 1]
    for index, part in enumerate(parts):
        e, f = split(potential[index])
        a, b = near[0, part, :], near[1, part, :]
        results.append((part, weight * (a * e - b * f), weight * (a * f + b * e)))
    return results


def scratch_of(plan):
    return [
        pltpu.VMEM((2 * plan.padded_tiles, LANES), F32),
        pltpu.VMEM((2, plan.kept, LANES), F32),
        pltpu.VMEM((2 * plan.kept, 2 * LANES), BF16),
    ]


def first_pair(plan):
    def body(own, near_in, kernel, left, right, twiddle, pair_in, accum, pair, tiles, near, fourier):
        results = exchange(plan, own, near_in[...], tiles, near, fourier, kernel, left, right, twiddle)
        for part, real, imag in results:
            accum[0, part, :] = real
            accum[1, part, :] = imag
        to_matrix(plan, pair_in[...], tiles, pair)

    matrix = jax.ShapeDtypeStruct((2, plan.kept, LANES), F32)
    return pl.pallas_call(
        body,
        out_shape=[matrix, matrix],
        in_specs=[VMEM] * 7,
        out_specs=[VMEM] * 2,
        scratch_shapes=scratch_of(plan),
        compiler_params=pltpu.CompilerParams(vmem_limit_bytes=16 * 1024 * 1024),
        name="first_pair",
    )


def second_pair(plan):
    def body(place, own, accum, far_in, near_in, kernel, left, right, twiddle, total, tiles, near, fourier):
        packed = jnp.where(place[0] % 2 == 1, near_in[...], far_in[...])
        results = exchange(plan, own, packed, tiles, near, fourier, kernel, left, right, twiddle)
        for part, real, imag in results:
            total[0, part, :] = (accum[0, part, :] + real).astype(BF16).astype(F32)
            total[1, part, :] = (accum[1, part, :] + imag).astype(BF16).astype(F32)

    return pl.pallas_call(
        body,
        out_shape=jax.ShapeDtypeStruct((2, plan.kept, LANES), F32),
        in_specs=[SMEM] + [VMEM] * 8,
        out_specs=VMEM,
        input_output_aliases={2: 0},
        scratch_shapes=scratch_of(plan),
        compiler_params=pltpu.CompilerParams(vmem_limit_bytes=16 * 1024 * 1024),
        name="second_pair",
    )


def finish(plan, others):
    count = others + 1

    def body(*refs):
        place, total, own, pair = refs[:4]
        bands = refs[4 : 3 + others]
        out, gram, tiles, matrix, flat, sent = refs[3 + others :]
        from_matrix(plan, total, tiles)
        for q in range(plan.tiles):
            turn, i = divmod(q, plan.tile_period)
            pair_rows = tiles[pl.ds(2 * plan.blocks * i + turn, 2, stride=plan.blocks), :].astype(BF16)
            used = min(LANES, plan.grid - LANES * q)
            if used:
                flat[:, LANES * q : LANES * q + used] = pair_rows[:, :used]
        copy = pltpu.make_async_copy(flat, out, sent)
        copy.start()
        here = place[0]

        @pl.when(here >= 0)
        def _():
            lane = lax.broadcasted_iota(jnp.int32, (1, count), 1)
            where = [here, here ^ 1]
            for step in range(1, count // 2):
                for start in (here, here ^ 1):
                    source = start - 2 * step
                    where.append(jnp.where(source < 0, source + count, source))
            sums = [jnp.zeros((1, count), F32)] * 2
            norm = 1.0 / math.sqrt(plan.grid)
            e = total[0]
            f = total[1]
            for index in range(count):
                if index < 2:
                    band = (own, pair)[index]
                    c, d = band[0], band[1]
                else:
                    to_matrix(plan, bands[index - 2][...], tiles, matrix)
                    c, d = matrix[0], matrix[1]
                parts = (c * e + d * f, c * f - d * e)
                for part in range(2):
                    value = jnp.sum(jnp.sum(parts[part], axis=0, keepdims=True), axis=1, keepdims=True)
                    sums[part] = jnp.where(lane == where[index], value * norm, sums[part])
            for part in range(2):
                gram[part] = sums[part]

        copy.wait()

    return pl.pallas_call(
        body,
        out_shape=[
            jax.ShapeDtypeStruct((2, plan.grid), BF16),
            jax.ShapeDtypeStruct((2, 1, count), F32),
        ],
        in_specs=[SMEM] + [VMEM] * (2 + others),
        out_specs=[ANYWHERE, VMEM],
        scratch_shapes=[
            pltpu.VMEM((2 * plan.padded_tiles, LANES), F32),
            pltpu.VMEM((2, plan.kept, LANES), F32),
            pltpu.VMEM((2, plan.grid), BF16),
            pltpu.SemaphoreType.DMA,
        ],
        compiler_params=pltpu.CompilerParams(vmem_limit_bytes=16 * 1024 * 1024),
        name="finish",
    )


def shards(orbitals, occupation, kernel):
    plan = Plan(orbitals.shape[3])
    pools = lax.axis_size("pool")
    groups = lax.axis_size("band")
    others = groups - 1

    def move(array, target):
        pairs = [
            (p * groups + g, q * groups + h)
            for p in range(pools)
            for g in range(groups)
            for q, h in [target(p, g)]
        ]
        return lax.ppermute(array, ("pool", "band"), pairs)

    here = lax.axis_index("band")
    place = lax.broadcast(here.astype(jnp.int32), (1,))
    own = pack(plan)(orbitals[0, 0], occupation[0])
    near = move(own, lambda p, g: ((p + 1) % pools, g))
    far = move(own, lambda p, g: ((p + 1) % pools, (g + 1) % groups) if g % 2 else (p, g + 1))
    partner = lambda p, g: (p, g ^ 1)
    bands = [move(own, partner)]
    for step in range(1, groups // 2):
        shifted = move(own, lambda p, g: (p, (g + 2 * step) % groups))
        crossed = move(shifted, partner)
        bands += [shifted, crossed]
    swapped = move(near, partner)
    tables = constants(plan)
    mine, factor = prepare(plan)(own, kernel, *tables)
    accum, pair = first_pair(plan)(mine, near, factor, *tables, bands[0])
    total = second_pair(plan)(
        place, mine, accum, far, swapped, factor, *tables
    )
    exchanged, gram = finish(plan, others)(place, total, mine, pair, *bands[1:])
    return exchanged[None, None], jnp.swapaxes(gram, 1, 2)[None]


def solution(mesh):
    return jax.shard_map(
        shards,
        mesh=mesh,
        in_specs=(P("pool", "band", None, None), P("pool", "band"), P()),
        out_specs=(P("pool", "band", None, None), P("pool", None, None, "band")),
        check_vma=False,
    )
```

```python
import math

import jax
import jax.numpy as jnp
import numpy as np
from jax import lax
from jax.experimental import pallas as pl
from jax.experimental.pallas import tpu as pltpu
from jax.sharding import PartitionSpec as P


LANES = 128
PARTS = 2
F32 = jnp.float32
BF16 = jnp.bfloat16
VMEM = pl.BlockSpec(memory_space=pltpu.VMEM)
SMEM = pl.BlockSpec(memory_space=pltpu.SMEM)
ANYWHERE = pl.BlockSpec(memory_space=pl.ANY)


class Plan:
    def __init__(self, grid):
        ng = round(grid ** (1.0 / 3.0))
        self.grid = grid
        self.ng = ng
        self.split = max(b for b in range(1, ng + 1) if ng % b == 0 and b * ng <= LANES)
        self.coarse = ng // self.split
        self.width = self.split * ng
        self.rows = grid // self.width
        self.tiles = grid // LANES + 1
        self.tail = grid % LANES
        common = math.lcm(self.width, LANES)
        self.row_period = common // self.width
        self.tile_period = common // LANES
        self.blocks = -(-self.rows // self.row_period)
        self.kept = self.blocks * self.row_period
        self.padded_tiles = (self.blocks * self.tile_period + 15) // 8 * 8


def roots(ng, phases):
    angles = 2.0 * np.pi / ng * (phases % ng)
    return np.cos(angles), np.sin(angles)


def constants(plan):
    ng, split, coarse, width = plan.ng, plan.split, plan.coarse, plan.width
    j, block = np.divmod(np.arange(plan.kept), plan.blocks)
    row = block * plan.row_period + j
    real_row = row < plan.rows
    x, a = np.divmod(row, coarse)
    b, z = np.divmod(np.arange(width), ng)
    mask = np.outer(real_row, real_row)
    cosine, sine = roots(ng, np.outer(x, x) + split * np.outer(a, a))
    left = np.concatenate([cosine * mask, sine * mask], axis=1)
    cosine, sine = roots(ng, coarse * np.outer(b, b) + np.outer(z, z))
    right = np.zeros((2, 2, LANES, 2, LANES))
    for way, sign in enumerate((1.0, -1.0)):
        right[way, 0, :width, 0, :width] = cosine
        right[way, 1, :width, 1, :width] = cosine
        right[way, 1, :width, 0, :width] = sign * sine
        right[way, 0, :width, 1, :width] = -sign * sine
    twiddle = np.zeros((2, plan.kept, LANES))
    twiddle[0, :, :width], twiddle[1, :, :width] = roots(ng, np.outer(a, b))
    return (
        jnp.asarray(left, BF16),
        jnp.asarray(right.reshape(2, 2 * LANES, 2 * LANES), BF16),
        jnp.asarray(twiddle, F32),
    )


def pack(plan):
    def body(orbital, occupation, out):
        last = plan.tiles - 1
        for q in range(last):
            out[2 * q : 2 * q + 2, :] = orbital[:, LANES * q : LANES * (q + 1)]
        if plan.tail:
            out[2 * last :, : plan.tail] = orbital[:, LANES * last :]
        fill = jnp.full((2, LANES - plan.tail), occupation[0], jnp.int32)
        out[2 * last :, plan.tail :] = fill.astype(F32).astype(BF16)

    return pl.pallas_call(
        body,
        out_shape=jax.ShapeDtypeStruct((2 * plan.tiles, LANES), BF16),
        in_specs=[VMEM, SMEM],
        out_specs=VMEM,
        compiler_params=pltpu.CompilerParams(vmem_limit_bytes=4 * 1024 * 1024),
        name="pack",
    )


def shifted_rows(plan, tiles, first, step, j):
    q, shift = divmod(plan.width * j, LANES)
    stride = step * plan.tile_period
    rows = tiles[pl.ds(step * q + first, plan.blocks, stride=stride), :]
    if shift + plan.width > LANES:
        after = tiles[pl.ds(step * (q + 1) + first, plan.blocks, stride=stride), :]
        lane = lax.broadcasted_iota(jnp.int32, rows.shape, 1)
        rows = jnp.where(lane >= shift, rows, after)
    return pltpu.roll(rows, LANES - shift, axis=1) if shift else rows


def to_matrix(plan, packed, tiles, matrix):
    size = 2 * plan.tiles
    tiles[:size, :] = packed.astype(F32)
    tiles[size:, :] = jnp.zeros((2 * plan.padded_tiles - size, LANES), F32)
    for j in range(plan.row_period):
        for part in range(2):
            rows = shifted_rows(plan, tiles, part, 2, j)
            matrix[part, plan.blocks * j : plan.blocks * (j + 1), :] = rows


def from_matrix(plan, matrix, tiles):
    width, blocks = plan.width, plan.blocks
    for i in range(plan.tile_period):
        for part in range(2):
            row, offset = divmod(LANES * i, width)
            flat = None
            start = -offset
            while start < LANES:
                turn, j = divmod(row, plan.row_period)
                rows = matrix[part, blocks * j + turn : blocks * (j + 1) + turn, :]
                if start % LANES:
                    rows = pltpu.roll(rows, start % LANES, axis=1)
                if flat is None:
                    flat = rows
                else:
                    lane = lax.broadcasted_iota(jnp.int32, rows.shape, 1)
                    flat = jnp.where(lane < start, flat, rows)
                start += width
                row += 1
            tiles[blocks * (2 * i + part) : blocks * (2 * i + part + 1), :] = flat


def prepare(plan):
    split, coarse, ng = plan.split, plan.coarse, plan.ng

    def body(own_in, kernel_in, left, right, twiddle, own, factor, tiles, plain, ordered):
        del left, right, twiddle
        to_matrix(plan, own_in[...], tiles, own)
        eight = 8 * LANES
        for q in range(0, plan.grid // eight):
            tiles[8 * q : 8 * q + 8, :] = kernel_in[eight * q : eight * (q + 1)].reshape(8, LANES)
        for q in range(plan.grid // eight * 8, plan.grid // LANES):
            tiles[q : q + 1, :] = kernel_in[LANES * q : LANES * (q + 1)].reshape(1, LANES)
        if plan.tail:
            q = plan.grid // LANES
            tiles[q : q + 1, : plan.tail] = kernel_in[LANES * q :].reshape(1, plan.tail)
        for j in range(plan.row_period):
            rows = shifted_rows(plan, tiles, 0, 1, j)
            plain[pl.ds(j, plan.blocks, stride=plan.row_period), :] = rows * (1.0 / plan.grid)
        lane = lax.broadcasted_iota(jnp.int32, (ng, LANES), 1)
        for a in range(coarse):
            rows = None
            for b in range(split):
                row, column = divmod(a + coarse * b, split)
                piece = plain[pl.ds(row, ng, stride=coarse), :]
                shift = (ng * (b - column)) % LANES
                if shift:
                    piece = pltpu.roll(piece, shift, axis=1)
                rows = piece if rows is None else jnp.where(lane < ng * b, rows, piece)
            ordered[pl.ds(a, ng, stride=coarse), :] = rows
        ordered[plan.rows :, :] = jnp.zeros((plan.kept - plan.rows, LANES), F32)
        for j in range(plan.row_period):
            rows = ordered[pl.ds(j, plan.blocks, stride=plan.row_period), :]
            factor[plan.blocks * j : plan.blocks * (j + 1), :] = rows

    return pl.pallas_call(
        body,
        out_shape=[
            jax.ShapeDtypeStruct((2, plan.kept, LANES), F32),
            jax.ShapeDtypeStruct((plan.kept, LANES), F32),
        ],
        in_specs=[VMEM] * 2 + [ANYWHERE] * 3,
        out_specs=[VMEM] * 2,
        scratch_shapes=[
            pltpu.VMEM((2 * plan.padded_tiles, LANES), F32),
            pltpu.VMEM((plan.kept, LANES), F32),
            pltpu.VMEM((plan.kept, LANES), F32),
        ],
        compiler_params=pltpu.CompilerParams(vmem_limit_bytes=4 * 1024 * 1024),
        name="prepare",
    )


def exchange(plan, own, packed, tiles, near, fourier, kernel, left, right, twiddle):
    rows = plan.kept
    to_matrix(plan, packed, tiles, near)
    c = own[0]
    d = own[1]
    a = near[0]
    b = near[1]

    step = rows // PARTS
    parts = [slice(step * index, step * (index + 1)) for index in range(PARTS)]

    def put(part, real, imag, sign):
        real = real.astype(BF16)
        imag = imag.astype(BF16)
        below = slice(rows + part.start, rows + part.stop)
        fourier[part, :LANES] = real
        fourier[part, LANES:] = imag
        fourier[below, :LANES] = imag if sign > 0 else -imag
        fourier[below, LANES:] = -real if sign > 0 else real

    def dot(x, y):
        return jnp.dot(x, y, preferred_element_type=F32)

    def split(value):
        return value[:, :LANES], value[:, LANES:]

    for part in parts:
        a, b, c, d = near[0, part, :], near[1, part, :], own[0, part, :], own[1, part, :]
        put(part, a * c + b * d, a * d - b * c, 1)
    halves = [dot(left[part, :], fourier[...]) for part in parts]
    for index, part in enumerate(parts):
        real, imag = split(halves[index])
        cosine, sine = twiddle[0, part, :], twiddle[1, part, :]
        halves[index] = jnp.concatenate(
            [real * cosine + imag * sine, imag * cosine - real * sine], axis=1
        ).astype(BF16)
    halves = [dot(value, right[0]) for value in halves]
    for index, part in enumerate(parts):
        real, imag = split(halves[index])
        factor = kernel[part, :]
        halves[index] = jnp.concatenate([real * factor, imag * factor], axis=1).astype(BF16)
    halves = [dot(value, right[1]) for value in halves]
    for index, part in enumerate(parts):
        real, imag = split(halves[index])
        cosine, sine = twiddle[0, part, :], twiddle[1, part, :]
        put(part, real * cosine - imag * sine, imag * cosine + real * sine, -1)
    potential = [dot(left[part, :], fourier[...]) for part in parts]
    results = []
    last = 2 * plan.tiles - 2
    weight = -0.5 * tiles[last : last + 1, plan.tail : plan.tail + 1]
    for index, part in enumerate(parts):
        e, f = split(potential[index])
        a, b = near[0, part, :], near[1, part, :]
        results.append((part, weight * (a * e - b * f), weight * (a * f + b * e)))
    return results


def scratch_of(plan):
    return [
        pltpu.VMEM((2 * plan.padded_tiles, LANES), F32),
        pltpu.VMEM((2, plan.kept, LANES), F32),
        pltpu.VMEM((2 * plan.kept, 2 * LANES), BF16),
    ]


def first_pair(plan):
    def body(own, near_in, kernel, left, right, twiddle, pair_in, accum, pair, tiles, near, fourier):
        results = exchange(plan, own, near_in[...], tiles, near, fourier, kernel, left, right, twiddle)
        for part, real, imag in results:
            accum[0, part, :] = real
            accum[1, part, :] = imag
        to_matrix(plan, pair_in[...], tiles, pair)

    matrix = jax.ShapeDtypeStruct((2, plan.kept, LANES), F32)
    return pl.pallas_call(
        body,
        out_shape=[matrix, matrix],
        in_specs=[VMEM] * 7,
        out_specs=[VMEM] * 2,
        scratch_shapes=scratch_of(plan),
        compiler_params=pltpu.CompilerParams(vmem_limit_bytes=16 * 1024 * 1024),
        name="first_pair",
    )


def second_pair(plan):
    def body(own, accum, far_in, near_in, kernel, left, right, twiddle, total, tiles, near, fourier):
        packed = jnp.where(lax.axis_index("band") % 2 == 1, near_in[...], far_in[...])
        results = exchange(plan, own, packed, tiles, near, fourier, kernel, left, right, twiddle)
        for part, real, imag in results:
            total[0, part, :] = (accum[0, part, :] + real).astype(BF16).astype(F32)
            total[1, part, :] = (accum[1, part, :] + imag).astype(BF16).astype(F32)

    return pl.pallas_call(
        body,
        out_shape=jax.ShapeDtypeStruct((2, plan.kept, LANES), F32),
        in_specs=[VMEM] * 8,
        out_specs=VMEM,
        input_output_aliases={1: 0},
        scratch_shapes=scratch_of(plan),
        compiler_params=pltpu.CompilerParams(vmem_limit_bytes=16 * 1024 * 1024),
        name="second_pair",
    )


def finish(plan, others):
    count = others + 1

    def body(*refs):
        total, own, pair = refs[:3]
        bands = refs[3 : 2 + others]
        out, gram, tiles, matrix, flat, sent = refs[2 + others :]
        from_matrix(plan, total, tiles)
        for q in range(plan.tiles):
            turn, i = divmod(q, plan.tile_period)
            pair_rows = tiles[pl.ds(2 * plan.blocks * i + turn, 2, stride=plan.blocks), :].astype(BF16)
            used = min(LANES, plan.grid - LANES * q)
            if used:
                flat[:, LANES * q : LANES * q + used] = pair_rows[:, :used]
        copy = pltpu.make_async_copy(flat, out, sent)
        copy.start()
        here = lax.axis_index("band")

        @pl.when(here >= 0)
        def _():
            lane = lax.broadcasted_iota(jnp.int32, (1, count), 1)
            where = [here, here ^ 1]
            for step in range(1, count // 2):
                for start in (here, here ^ 1):
                    source = start - 2 * step
                    where.append(jnp.where(source < 0, source + count, source))
            sums = [jnp.zeros((1, count), F32)] * 2
            norm = 1.0 / math.sqrt(plan.grid)
            e = total[0]
            f = total[1]
            for index in range(count):
                if index < 2:
                    band = (own, pair)[index]
                    c, d = band[0], band[1]
                else:
                    to_matrix(plan, bands[index - 2][...], tiles, matrix)
                    c, d = matrix[0], matrix[1]
                parts = (c * e + d * f, c * f - d * e)
                for part in range(2):
                    value = jnp.sum(jnp.sum(parts[part], axis=0, keepdims=True), axis=1, keepdims=True)
                    sums[part] = jnp.where(lane == where[index], value * norm, sums[part])
            for part in range(2):
                gram[part] = sums[part]

        copy.wait()

    return pl.pallas_call(
        body,
        out_shape=[
            jax.ShapeDtypeStruct((2, plan.grid), BF16),
            jax.ShapeDtypeStruct((2, 1, count), F32),
        ],
        in_specs=[VMEM] * (2 + others),
        out_specs=[ANYWHERE, VMEM],
        scratch_shapes=[
            pltpu.VMEM((2 * plan.padded_tiles, LANES), F32),
            pltpu.VMEM((2, plan.kept, LANES), F32),
            pltpu.VMEM((2, plan.grid), BF16),
            pltpu.SemaphoreType.DMA,
        ],
        compiler_params=pltpu.CompilerParams(vmem_limit_bytes=16 * 1024 * 1024),
        name="finish",
    )


def shards(orbitals, occupation, kernel):
    plan = Plan(orbitals.shape[3])
    pools = lax.axis_size("pool")
    groups = lax.axis_size("band")
    others = groups - 1

    def move(array, target):
        pairs = [
            (p * groups + g, q * groups + h)
            for p in range(pools)
            for g in range(groups)
            for q, h in [target(p, g)]
        ]
        return lax.ppermute(array, ("pool", "band"), pairs)

    own = pack(plan)(orbitals[0, 0], occupation[0])
    near = move(own, lambda p, g: ((p + 1) % pools, g))
    far = move(own, lambda p, g: ((p + 1) % pools, (g + 1) % groups) if g % 2 else (p, g + 1))
    partner = lambda p, g: (p, g ^ 1)
    bands = [move(own, partner)]
    for step in range(1, groups // 2):
        shifted = move(own, lambda p, g: (p, (g + 2 * step) % groups))
        crossed = move(shifted, partner)
        bands += [shifted, crossed]
    swapped = move(near, partner)
    tables = constants(plan)
    mine, factor = prepare(plan)(own, kernel, *tables)
    accum, pair = first_pair(plan)(mine, near, factor, *tables, bands[0])
    total = second_pair(plan)(
        mine, accum, far, swapped, factor, *tables
    )
    exchanged, gram = finish(plan, others)(total, mine, pair, *bands[1:])
    return exchanged[None, None], jnp.swapaxes(gram, 1, 2)[None]


def solution(mesh):
    return jax.shard_map(
        shards,
        mesh=mesh,
        in_specs=(P("pool", "band", None, None), P("pool", "band"), P()),
        out_specs=(P("pool", "band", None, None), P("pool", None, None, "band")),
        check_vma=False,
    )
```

```python
import math

import jax
import jax.numpy as jnp
import numpy as np
from jax import lax
from jax.experimental import pallas as pl
from jax.experimental.pallas import tpu as pltpu
from jax.sharding import PartitionSpec as P


LANES = 128
F32 = jnp.float32
BF16 = jnp.bfloat16
VMEM = pl.BlockSpec(memory_space=pltpu.VMEM)
SMEM = pl.BlockSpec(memory_space=pltpu.SMEM)
ANYWHERE = pl.BlockSpec(memory_space=pl.ANY)


class Plan:
    def __init__(self, grid):
        ng = round(grid ** (1.0 / 3.0))
        self.grid = grid
        self.ng = ng
        self.split = max(b for b in range(1, ng + 1) if ng % b == 0 and b * ng <= LANES)
        self.coarse = ng // self.split
        self.width = self.split * ng
        self.rows = grid // self.width
        self.tiles = grid // LANES + 1
        self.tail = grid % LANES
        common = math.lcm(self.width, LANES)
        self.row_period = common // self.width
        self.tile_period = common // LANES
        self.blocks = -(-self.rows // self.row_period)
        self.half = self.rows // 2
        self.half_blocks = -(-self.half // self.row_period)
        self.half_kept = self.half_blocks * self.row_period
        self.kept = 2 * self.half_kept
        self.padded_tiles = (self.blocks * self.tile_period + 15) // 8 * 8


def roots(ng, phases):
    angles = 2.0 * np.pi / ng * (phases % ng)
    return np.cos(angles), np.sin(angles)


def constants(plan):
    ng, split, coarse, width = plan.ng, plan.split, plan.coarse, plan.width
    j, block = np.divmod(np.arange(plan.half_kept), plan.half_blocks)
    row = block * plan.row_period + j
    real_row = row < plan.half
    x, a = np.divmod(row, coarse)
    b, z = np.divmod(np.arange(width), ng)
    mask = np.outer(real_row, real_row)
    left = []
    for first, second in ((2 * x, x), (2 * x + 1, x), (x, 2 * x + 1)):
        cosine, sine = roots(ng, np.outer(first, second) + split * np.outer(a, a))
        left.append(np.concatenate([cosine * mask, sine * mask], axis=1))
    left = np.stack(left)
    cosine, sine = roots(ng, coarse * np.outer(b, b) + np.outer(z, z))
    right = np.zeros((2, 2, LANES, 2, LANES))
    for way, sign in enumerate((1.0, -1.0)):
        right[way, 0, :width, 0, :width] = cosine
        right[way, 1, :width, 1, :width] = cosine
        right[way, 1, :width, 0, :width] = sign * sine
        right[way, 0, :width, 1, :width] = -sign * sine
    twiddle = np.zeros((2, plan.half_kept, LANES))
    twiddle[0, :, :width], twiddle[1, :, :width] = roots(ng, np.outer(a, b))
    return (
        jnp.asarray(left, BF16),
        jnp.asarray(right.reshape(2, 2 * LANES, 2 * LANES), BF16),
        jnp.asarray(twiddle, F32),
    )


def pack(plan):
    def body(orbital, occupation, out):
        last = plan.tiles - 1
        for q in range(last):
            out[2 * q : 2 * q + 2, :] = orbital[:, LANES * q : LANES * (q + 1)]
        if plan.tail:
            out[2 * last :, : plan.tail] = orbital[:, LANES * last :]
        fill = jnp.full((2, LANES - plan.tail), occupation[0], jnp.int32)
        out[2 * last :, plan.tail :] = fill.astype(F32).astype(BF16)

    return pl.pallas_call(
        body,
        out_shape=jax.ShapeDtypeStruct((2 * plan.tiles, LANES), BF16),
        in_specs=[VMEM, SMEM],
        out_specs=VMEM,
        compiler_params=pltpu.CompilerParams(vmem_limit_bytes=4 * 1024 * 1024),
        name="pack",
    )


def shifted_rows(plan, tiles, first, step, row, count):
    q, shift = divmod(plan.width * row, LANES)
    stride = step * plan.tile_period
    rows = tiles[pl.ds(step * q + first, count, stride=stride), :]
    if shift + plan.width > LANES:
        after = tiles[pl.ds(step * (q + 1) + first, count, stride=stride), :]
        lane = lax.broadcasted_iota(jnp.int32, rows.shape, 1)
        rows = jnp.where(lane >= shift, rows, after)
    return pltpu.roll(rows, LANES - shift, axis=1) if shift else rows


def to_matrix(plan, packed, tiles, matrix):
    size = 2 * plan.tiles
    tiles[:size, :] = packed.astype(F32)
    tiles[size:, :] = jnp.zeros((2 * plan.padded_tiles - size, LANES), F32)
    count = plan.half_blocks
    for upper in range(2):
        for j in range(plan.row_period):
            first = plan.half_kept * upper + count * j
            for part in range(2):
                rows = shifted_rows(plan, tiles, part, 2, j + plan.half * upper, count)
                matrix[part, first : first + count, :] = rows


def join_halves(plan, matrix, whole):
    for upper in range(2):
        for j in range(plan.row_period):
            count = -(-(plan.half - j) // plan.row_period)
            source = plan.half_kept * upper + plan.half_blocks * j
            turn, place = divmod(j + plan.half * upper, plan.row_period)
            target = plan.blocks * place + turn
            for part in range(2):
                whole[part, target : target + count, :] = matrix[part, source : source + count, :]


def from_matrix(plan, matrix, tiles):
    width, blocks = plan.width, plan.blocks
    for i in range(plan.tile_period):
        for part in range(2):
            row, offset = divmod(LANES * i, width)
            flat = None
            start = -offset
            while start < LANES:
                turn, j = divmod(row, plan.row_period)
                rows = matrix[part, blocks * j + turn : blocks * (j + 1) + turn, :]
                if start % LANES:
                    rows = pltpu.roll(rows, start % LANES, axis=1)
                if flat is None:
                    flat = rows
                else:
                    lane = lax.broadcasted_iota(jnp.int32, rows.shape, 1)
                    flat = jnp.where(lane < start, flat, rows)
                start += width
                row += 1
            tiles[blocks * (2 * i + part) : blocks * (2 * i + part + 1), :] = flat


def prepare(plan):
    split, coarse, ng = plan.split, plan.coarse, plan.ng

    def body(own_in, pair_in, kernel_in, left, right, twiddle, own, pair, factor, tiles, plain, ordered):
        del left, right, twiddle
        to_matrix(plan, own_in[...], tiles, own)
        to_matrix(plan, pair_in[...], tiles, pair)
        eight = 8 * LANES
        for q in range(0, plan.grid // eight):
            tiles[8 * q : 8 * q + 8, :] = kernel_in[eight * q : eight * (q + 1)].reshape(8, LANES)
        for q in range(plan.grid // eight * 8, plan.grid // LANES):
            tiles[q : q + 1, :] = kernel_in[LANES * q : LANES * (q + 1)].reshape(1, LANES)
        if plan.tail:
            q = plan.grid // LANES
            tiles[q : q + 1, : plan.tail] = kernel_in[LANES * q :].reshape(1, plan.tail)
        for j in range(plan.row_period):
            rows = shifted_rows(plan, tiles, 0, 1, j, plan.blocks)
            plain[pl.ds(j, plan.blocks, stride=plan.row_period), :] = rows * (1.0 / plan.grid)
        count = ng // 2
        lane = lax.broadcasted_iota(jnp.int32, (count, LANES), 1)
        for odd in range(2):
            base = plan.half_kept * odd
            for a in range(coarse):
                rows = None
                for b in range(split):
                    row, column = divmod(a + coarse * b, split)
                    piece = plain[pl.ds(coarse * odd + row, count, stride=2 * coarse), :]
                    shift = (ng * (b - column)) % LANES
                    if shift:
                        piece = pltpu.roll(piece, shift, axis=1)
                    rows = piece if rows is None else jnp.where(lane < ng * b, rows, piece)
                ordered[pl.ds(base + a, count, stride=coarse), :] = rows
            spare = plan.half_kept - plan.half
            if spare:
                ordered[base + plan.half : base + plan.half_kept, :] = jnp.zeros((spare, LANES), F32)
            for j in range(plan.row_period):
                rows = ordered[pl.ds(base + j, plan.half_blocks, stride=plan.row_period), :]
                first = base + plan.half_blocks * j
                factor[first : first + plan.half_blocks, :] = rows

    return pl.pallas_call(
        body,
        out_shape=[
            jax.ShapeDtypeStruct((2, plan.kept, LANES), F32),
            jax.ShapeDtypeStruct((2, plan.kept, LANES), F32),
            jax.ShapeDtypeStruct((plan.kept, LANES), F32),
        ],
        in_specs=[VMEM] * 3 + [ANYWHERE] * 3,
        out_specs=[VMEM] * 3,
        scratch_shapes=[
            pltpu.VMEM((2 * plan.padded_tiles, LANES), F32),
            pltpu.VMEM((plan.blocks * plan.row_period, LANES), F32),
            pltpu.VMEM((plan.kept, LANES), F32),
        ],
        compiler_params=pltpu.CompilerParams(vmem_limit_bytes=4 * 1024 * 1024),
        name="prepare",
    )


def exchange(plan, own, packed, tiles, near, fourier, kernel, left, right, twiddle):
    to_matrix(plan, packed, tiles, near)
    size = plan.half_kept
    parts = [slice(0, size), slice(size, 2 * size)]

    def put(index, real, imag, sign):
        real = real.astype(BF16)
        imag = imag.astype(BF16)
        above = slice(2 * size * index, 2 * size * index + size)
        below = slice(2 * size * index + size, 2 * size * (index + 1))
        fourier[above, :LANES] = real
        fourier[above, LANES:] = imag
        fourier[below, :LANES] = imag if sign > 0 else -imag
        fourier[below, LANES:] = -real if sign > 0 else real

    def dot(x, y):
        return jnp.dot(x, y, preferred_element_type=F32)

    def both(tables):
        return [
            dot(left[table], fourier[2 * size * index : 2 * size * (index + 1), :])
            for index, table in enumerate(tables)
        ]

    def halve(value):
        return value[:, :LANES], value[:, LANES:]

    density = []
    for part in parts:
        a, b, c, d = near[0, part, :], near[1, part, :], own[0, part, :], own[1, part, :]
        density.append((a * c + b * d, a * d - b * c))
    (low_real, low_imag), (high_real, high_imag) = density
    put(0, low_real + high_real, low_imag + high_imag, 1)
    put(1, low_real - high_real, low_imag - high_imag, 1)
    values = both((0, 1))
    cosine, sine = twiddle[0], twiddle[1]
    for index in range(2):
        real, imag = halve(values[index])
        values[index] = jnp.concatenate(
            [real * cosine + imag * sine, imag * cosine - real * sine], axis=1
        ).astype(BF16)
    values = [dot(value, right[0]) for value in values]
    for index, part in enumerate(parts):
        real, imag = halve(values[index])
        factor = kernel[part, :]
        values[index] = jnp.concatenate([real * factor, imag * factor], axis=1).astype(BF16)
    values = [dot(value, right[1]) for value in values]
    for index in range(2):
        real, imag = halve(values[index])
        put(index, real * cosine - imag * sine, imag * cosine + real * sine, -1)
    even, odd = both((0, 2))
    potential = [even + odd, even - odd]
    results = []
    last = 2 * plan.tiles - 2
    weight = -0.5 * tiles[last : last + 1, plan.tail : plan.tail + 1]
    for index, part in enumerate(parts):
        e, f = halve(potential[index])
        a, b = near[0, part, :], near[1, part, :]
        results.append((part, weight * (a * e - b * f), weight * (a * f + b * e)))
    return results


def scratch_of(plan):
    whole = max(plan.kept, plan.blocks * plan.row_period)
    return [
        pltpu.VMEM((2 * plan.padded_tiles, LANES), F32),
        pltpu.VMEM((2, whole, LANES), F32),
        pltpu.VMEM((2 * plan.kept, 2 * LANES), BF16),
    ]


def first_pair(plan, extra):
    def body(*refs):
        own, near_in, kernel, left, right, twiddle = refs[:6]
        bands = refs[6 : 6 + extra]
        accum, *matrices, tiles, near, fourier = refs[6 + extra :]
        results = exchange(plan, own, near_in[...], tiles, near, fourier, kernel, left, right, twiddle)
        for part, real, imag in results:
            accum[0, part, :] = real
            accum[1, part, :] = imag
        for band, matrix in zip(bands, matrices):
            to_matrix(plan, band[...], tiles, matrix)

    matrix = jax.ShapeDtypeStruct((2, plan.kept, LANES), F32)
    return pl.pallas_call(
        body,
        out_shape=[matrix] * (1 + extra),
        in_specs=[VMEM] * (6 + extra),
        out_specs=[VMEM] * (1 + extra),
        scratch_shapes=scratch_of(plan),
        compiler_params=pltpu.CompilerParams(vmem_limit_bytes=16 * 1024 * 1024),
        name="first_pair",
    )


def overlaps(plan, count, total, bands):
    lane = lax.broadcasted_iota(jnp.int32, (1, count), 1)
    norm = 1.0 / math.sqrt(plan.grid)
    sums = [jnp.zeros((1, count), F32)] * 2
    e, f = total[0], total[1]
    for place, band in bands:
        c, d = band[0], band[1]
        parts = (c * e + d * f, c * f - d * e)
        for part in range(2):
            value = jnp.sum(jnp.sum(parts[part], axis=0, keepdims=True), axis=1, keepdims=True)
            sums[part] = jnp.where(lane == place, value * norm, sums[part])
    return sums


def second_pair(plan, others):
    count = others + 1

    def body(*refs):
        own, accum, far_in, near_in, kernel, left, right, twiddle, pair = refs[:9]
        extra = (others - 1) // 2
        shifted = refs[9 : 9 + extra]
        crossed = refs[9 + extra : 9 + 2 * extra]
        out, gram, tiles, near, fourier, total, flat, small, sent, spare, *matrices = refs[8 + others :]
        here = lax.axis_index("band")
        packed = jnp.where(here % 2 == 1, near_in[...], far_in[...])
        for band, matrix in zip(crossed, matrices):
            to_matrix(plan, band[...], spare, matrix)
        results = exchange(plan, own, packed, tiles, near, fourier, kernel, left, right, twiddle)
        for part, real, imag in results:
            total[0, part, :] = (accum[0, part, :] + real).astype(BF16).astype(F32)
            total[1, part, :] = (accum[1, part, :] + imag).astype(BF16).astype(F32)
        join_halves(plan, total, near)
        from_matrix(plan, near, tiles)
        for q in range(plan.tiles):
            turn, i = divmod(q, plan.tile_period)
            rows = tiles[pl.ds(2 * plan.blocks * i + turn, 2, stride=plan.blocks), :].astype(BF16)
            used = min(LANES, plan.grid - LANES * q)
            if used:
                flat[:, LANES * q : LANES * q + used] = rows[:, :used]
        copies = [
            pltpu.make_async_copy(flat, out, sent.at[0]),
            pltpu.make_async_copy(small, gram, sent.at[1]),
        ]
        copies[0].start()

        @pl.when(here >= 0)
        def _():
            pairs = [(here, own), (here ^ 1, pair)]
            for step in range(1, count // 2):
                for start, matrix in ((here, shifted[step - 1]), (here ^ 1, matrices[step - 1])):
                    source = start - 2 * step
                    pairs.append((jnp.where(source < 0, source + count, source), matrix))
            sums = overlaps(plan, count, total, pairs)
            for part in range(2):
                small[part] = sums[part]

        copies[1].start()
        for copy in copies:
            copy.wait()

    return pl.pallas_call(
        body,
        out_shape=[
            jax.ShapeDtypeStruct((2, plan.grid), BF16),
            jax.ShapeDtypeStruct((2, 1, count), F32),
        ],
        in_specs=[VMEM] * (8 + others),
        out_specs=[ANYWHERE] * 2,
        scratch_shapes=scratch_of(plan)
        + [
            pltpu.VMEM((2, plan.kept, LANES), F32),
            pltpu.VMEM((2, plan.grid), BF16),
            pltpu.VMEM((2, 1, count), F32),
            pltpu.SemaphoreType.DMA((2,)),
            pltpu.VMEM((2 * plan.padded_tiles, LANES), F32),
        ]
        + [pltpu.VMEM((2, plan.kept, LANES), F32)] * ((others - 1) // 2),
        compiler_params=pltpu.CompilerParams(vmem_limit_bytes=16 * 1024 * 1024),
        name="second_pair",
    )


def shards(orbitals, occupation, kernel):
    plan = Plan(orbitals.shape[3])
    pools = lax.axis_size("pool")
    groups = lax.axis_size("band")
    others = groups - 1

    def move(array, target):
        pairs = [
            (p * groups + g, q * groups + h)
            for p in range(pools)
            for g in range(groups)
            for q, h in [target(p, g)]
        ]
        return lax.ppermute(array, ("pool", "band"), pairs)

    own = pack(plan)(orbitals[0, 0], occupation[0])
    near = move(own, lambda p, g: ((p + 1) % pools, g))
    far = move(own, lambda p, g: ((p + 1) % pools, (g + 1) % groups) if g % 2 else (p, g + 1))
    partner = lambda p, g: (p, g ^ 1)
    pair_in = move(own, partner)
    shifted, crossed = [], []
    for step in range(1, groups // 2):
        shifted.append(move(own, lambda p, g: (p, (g + 2 * step) % groups)))
        crossed.append(move(shifted[-1], partner))
    swapped = move(near, partner)
    tables = constants(plan)
    mine, pair, factor = prepare(plan)(own, pair_in, kernel, *tables)
    accum, *matrices = first_pair(plan, len(shifted))(
        mine, near, factor, *tables, *shifted
    )
    exchanged, gram = second_pair(plan, others)(
        mine, accum, far, swapped, factor, *tables, pair, *matrices, *crossed
    )
    return exchanged[None, None], jnp.swapaxes(gram, 1, 2)[None]


def solution(mesh):
    return jax.shard_map(
        shards,
        mesh=mesh,
        in_specs=(P("pool", "band", None, None), P("pool", "band"), P()),
        out_specs=(P("pool", "band", None, None), P("pool", None, None, "band")),
        check_vma=False,
    )
```

```python
import math

import jax
import jax.numpy as jnp
import numpy as np
from jax import lax
from jax.experimental import pallas as pl
from jax.experimental.pallas import tpu as pltpu
from jax.sharding import PartitionSpec as P


LANES = 128
F32 = jnp.float32
BF16 = jnp.bfloat16
VMEM = pl.BlockSpec(memory_space=pltpu.VMEM)
SMEM = pl.BlockSpec(memory_space=pltpu.SMEM)
ANYWHERE = pl.BlockSpec(memory_space=pl.ANY)


class Plan:
    def __init__(self, grid):
        ng = round(grid ** (1.0 / 3.0))
        self.grid = grid
        self.ng = ng
        self.split = max(b for b in range(1, ng + 1) if ng % b == 0 and b * ng <= LANES)
        self.coarse = ng // self.split
        self.width = self.split * ng
        self.rows = grid // self.width
        self.tiles = grid // LANES + 1
        self.tail = grid % LANES
        common = math.lcm(self.width, LANES)
        self.row_period = common // self.width
        self.tile_period = common // LANES
        self.blocks = -(-self.rows // self.row_period)
        self.half = self.rows // 2
        self.half_blocks = -(-self.half // self.row_period)
        self.half_kept = self.half_blocks * self.row_period
        self.kept = 2 * self.half_kept
        self.padded_tiles = (self.blocks * self.tile_period + 15) // 8 * 8


def roots(ng, phases):
    angles = 2.0 * np.pi / ng * (phases % ng)
    return np.cos(angles), np.sin(angles)


def constants(plan):
    ng, split, coarse, width = plan.ng, plan.split, plan.coarse, plan.width
    j, block = np.divmod(np.arange(plan.half_kept), plan.half_blocks)
    row = block * plan.row_period + j
    real_row = row < plan.half
    x, a = np.divmod(row, coarse)
    b, z = np.divmod(np.arange(width), ng)
    mask = np.outer(real_row, real_row)
    left = []
    for first, second in ((2 * x, x), (2 * x + 1, x), (x, 2 * x + 1)):
        cosine, sine = roots(ng, np.outer(first, second) + split * np.outer(a, a))
        left.append(np.concatenate([cosine * mask, sine * mask], axis=1))
    left = np.stack(left)
    cosine, sine = roots(ng, coarse * np.outer(b, b) + np.outer(z, z))
    right = np.zeros((2, 2, LANES, 2, LANES))
    for way, sign in enumerate((1.0, -1.0)):
        right[way, 0, :width, 0, :width] = cosine
        right[way, 1, :width, 1, :width] = cosine
        right[way, 1, :width, 0, :width] = sign * sine
        right[way, 0, :width, 1, :width] = -sign * sine
    twiddle = np.zeros((2, plan.half_kept, LANES))
    twiddle[0, :, :width], twiddle[1, :, :width] = roots(ng, np.outer(a, b))
    return (
        jnp.asarray(left, BF16),
        jnp.asarray(right.reshape(2, 2 * LANES, 2 * LANES), BF16),
        jnp.asarray(twiddle, F32),
    )


def pack(plan):
    def body(orbital, occupation, out):
        last = plan.tiles - 1
        for q in range(last):
            out[2 * q : 2 * q + 2, :] = orbital[:, LANES * q : LANES * (q + 1)]
        if plan.tail:
            out[2 * last :, : plan.tail] = orbital[:, LANES * last :]
        fill = jnp.full((2, LANES - plan.tail), occupation[0], jnp.int32)
        out[2 * last :, plan.tail :] = fill.astype(F32).astype(BF16)

    return pl.pallas_call(
        body,
        out_shape=jax.ShapeDtypeStruct((2 * plan.tiles, LANES), BF16),
        in_specs=[VMEM, SMEM],
        out_specs=VMEM,
        compiler_params=pltpu.CompilerParams(vmem_limit_bytes=4 * 1024 * 1024),
        name="pack",
    )


def shifted_rows(plan, tiles, first, step, row, count):
    q, shift = divmod(plan.width * row, LANES)
    stride = step * plan.tile_period
    rows = tiles[pl.ds(step * q + first, count, stride=stride), :]
    if shift + plan.width > LANES:
        after = tiles[pl.ds(step * (q + 1) + first, count, stride=stride), :]
        lane = lax.broadcasted_iota(jnp.int32, rows.shape, 1)
        rows = jnp.where(lane >= shift, rows, after)
    return pltpu.roll(rows, LANES - shift, axis=1) if shift else rows


def to_matrix(plan, packed, tiles, matrix):
    size = 2 * plan.tiles
    tiles[:size, :] = packed.astype(F32)
    tiles[size:, :] = jnp.zeros((2 * plan.padded_tiles - size, LANES), F32)
    count = plan.half_blocks
    for upper in range(2):
        for j in range(plan.row_period):
            first = plan.half_kept * upper + count * j
            for part in range(2):
                rows = shifted_rows(plan, tiles, part, 2, j + plan.half * upper, count)
                matrix[part, first : first + count, :] = rows


def join_halves(plan, matrix, whole):
    for upper in range(2):
        for j in range(plan.row_period):
            count = -(-(plan.half - j) // plan.row_period)
            source = plan.half_kept * upper + plan.half_blocks * j
            turn, place = divmod(j + plan.half * upper, plan.row_period)
            target = plan.blocks * place + turn
            for part in range(2):
                whole[part, target : target + count, :] = matrix[part, source : source + count, :]


def from_matrix(plan, matrix, tiles):
    width, blocks = plan.width, plan.blocks
    for i in range(plan.tile_period):
        for part in range(2):
            row, offset = divmod(LANES * i, width)
            flat = None
            start = -offset
            while start < LANES:
                turn, j = divmod(row, plan.row_period)
                rows = matrix[part, blocks * j + turn : blocks * (j + 1) + turn, :]
                if start % LANES:
                    rows = pltpu.roll(rows, start % LANES, axis=1)
                if flat is None:
                    flat = rows
                else:
                    lane = lax.broadcasted_iota(jnp.int32, rows.shape, 1)
                    flat = jnp.where(lane < start, flat, rows)
                start += width
                row += 1
            tiles[blocks * (2 * i + part) : blocks * (2 * i + part + 1), :] = flat


def prepare(plan):
    split, coarse, ng = plan.split, plan.coarse, plan.ng

    def body(own_in, pair_in, kernel_in, left, right, twiddle, own, pair, factor, tiles, plain, ordered):
        del left, right, twiddle
        to_matrix(plan, own_in[...], tiles, own)
        to_matrix(plan, pair_in[...], tiles, pair)
        eight = 8 * LANES
        for q in range(0, plan.grid // eight):
            tiles[8 * q : 8 * q + 8, :] = kernel_in[eight * q : eight * (q + 1)].reshape(8, LANES)
        for q in range(plan.grid // eight * 8, plan.grid // LANES):
            tiles[q : q + 1, :] = kernel_in[LANES * q : LANES * (q + 1)].reshape(1, LANES)
        if plan.tail:
            q = plan.grid // LANES
            tiles[q : q + 1, : plan.tail] = kernel_in[LANES * q :].reshape(1, plan.tail)
        for j in range(plan.row_period):
            rows = shifted_rows(plan, tiles, 0, 1, j, plan.blocks)
            plain[pl.ds(j, plan.blocks, stride=plan.row_period), :] = rows * (1.0 / plan.grid)
        count = ng // 2
        lane = lax.broadcasted_iota(jnp.int32, (count, LANES), 1)
        for odd in range(2):
            base = plan.half_kept * odd
            for a in range(coarse):
                rows = None
                for b in range(split):
                    row, column = divmod(a + coarse * b, split)
                    piece = plain[pl.ds(coarse * odd + row, count, stride=2 * coarse), :]
                    shift = (ng * (b - column)) % LANES
                    if shift:
                        piece = pltpu.roll(piece, shift, axis=1)
                    rows = piece if rows is None else jnp.where(lane < ng * b, rows, piece)
                ordered[pl.ds(base + a, count, stride=coarse), :] = rows
            spare = plan.half_kept - plan.half
            if spare:
                ordered[base + plan.half : base + plan.half_kept, :] = jnp.zeros((spare, LANES), F32)
            for j in range(plan.row_period):
                rows = ordered[pl.ds(base + j, plan.half_blocks, stride=plan.row_period), :]
                first = base + plan.half_blocks * j
                factor[first : first + plan.half_blocks, :] = rows

    return pl.pallas_call(
        body,
        out_shape=[
            jax.ShapeDtypeStruct((2, plan.kept, LANES), F32),
            jax.ShapeDtypeStruct((2, plan.kept, LANES), F32),
            jax.ShapeDtypeStruct((plan.kept, LANES), F32),
        ],
        in_specs=[VMEM] * 3 + [ANYWHERE] * 3,
        out_specs=[VMEM] * 3,
        scratch_shapes=[
            pltpu.VMEM((2 * plan.padded_tiles, LANES), F32),
            pltpu.VMEM((plan.blocks * plan.row_period, LANES), F32),
            pltpu.VMEM((plan.kept, LANES), F32),
        ],
        compiler_params=pltpu.CompilerParams(vmem_limit_bytes=4 * 1024 * 1024),
        name="prepare",
    )


def exchange(plan, own, packed, tiles, near, fourier, kernel, left, right, twiddle):
    to_matrix(plan, packed, tiles, near)
    size = plan.half_kept
    parts = [slice(0, size), slice(size, 2 * size)]

    def put(index, real, imag, sign):
        real = real.astype(BF16)
        imag = imag.astype(BF16)
        above = slice(2 * size * index, 2 * size * index + size)
        below = slice(2 * size * index + size, 2 * size * (index + 1))
        fourier[above, :LANES] = real
        fourier[above, LANES:] = imag
        fourier[below, :LANES] = imag if sign > 0 else -imag
        fourier[below, LANES:] = -real if sign > 0 else real

    def dot(x, y):
        return jnp.dot(x, y, preferred_element_type=F32)

    def both(tables):
        return [
            dot(left[table], fourier[2 * size * index : 2 * size * (index + 1), :])
            for index, table in enumerate(tables)
        ]

    def halve(value):
        return value[:, :LANES], value[:, LANES:]

    density = []
    for part in parts:
        a, b, c, d = near[0, part, :], near[1, part, :], own[0, part, :], own[1, part, :]
        density.append((a * c + b * d, a * d - b * c))
    (low_real, low_imag), (high_real, high_imag) = density
    put(0, low_real + high_real, low_imag + high_imag, 1)
    put(1, low_real - high_real, low_imag - high_imag, 1)
    values = both((0, 1))
    cosine, sine = twiddle[0], twiddle[1]
    for index in range(2):
        real, imag = halve(values[index])
        values[index] = jnp.concatenate(
            [real * cosine + imag * sine, imag * cosine - real * sine], axis=1
        ).astype(BF16)
    values = [dot(value, right[0]) for value in values]
    for index, part in enumerate(parts):
        real, imag = halve(values[index])
        factor = kernel[part, :]
        values[index] = jnp.concatenate([real * factor, imag * factor], axis=1).astype(BF16)
    values = [dot(value, right[1]) for value in values]
    for index in range(2):
        real, imag = halve(values[index])
        put(index, real * cosine - imag * sine, imag * cosine + real * sine, -1)
    even, odd = both((0, 2))
    potential = [even + odd, even - odd]
    results = []
    last = 2 * plan.tiles - 2
    weight = -0.5 * tiles[last : last + 1, plan.tail : plan.tail + 1]
    for index, part in enumerate(parts):
        e, f = halve(potential[index])
        a, b = near[0, part, :], near[1, part, :]
        results.append((part, weight * (a * e - b * f), weight * (a * f + b * e)))
    return results


def scratch_of(plan):
    whole = max(plan.kept, plan.blocks * plan.row_period)
    return [
        pltpu.VMEM((2 * plan.padded_tiles, LANES), F32),
        pltpu.VMEM((2, whole, LANES), F32),
        pltpu.VMEM((2 * plan.kept, 2 * LANES), BF16),
    ]


def first_pair(plan, extra):
    def body(*refs):
        own, near_in, kernel, left, right, twiddle = refs[:6]
        bands = refs[6 : 6 + extra]
        accum, *matrices, tiles, near, fourier = refs[6 + extra :]
        results = exchange(plan, own, near_in[...], tiles, near, fourier, kernel, left, right, twiddle)
        for part, real, imag in results:
            accum[0, part, :] = real
            accum[1, part, :] = imag
        for band, matrix in zip(bands, matrices):
            to_matrix(plan, band[...], tiles, matrix)

    matrix = jax.ShapeDtypeStruct((2, plan.kept, LANES), F32)
    return pl.pallas_call(
        body,
        out_shape=[matrix] * (1 + extra),
        in_specs=[VMEM] * (6 + extra),
        out_specs=[VMEM] * (1 + extra),
        scratch_shapes=scratch_of(plan),
        compiler_params=pltpu.CompilerParams(vmem_limit_bytes=16 * 1024 * 1024),
        name="first_pair",
    )


def overlaps(plan, count, total, bands):
    step = 56 if plan.kept % 56 == 0 else 8
    sums = [jnp.zeros((8, LANES), F32)] * (2 * count)
    for first in range(0, plan.kept, step):
        rows = slice(first, first + step)
        e, f = total[0, rows, :], total[1, rows, :]
        for index, (_, band) in enumerate(bands):
            c, d = band[0, rows, :], band[1, rows, :]
            for part, value in enumerate((c * e + d * f, c * f - d * e)):
                value = jnp.sum(value.reshape(step // 8, 8, LANES), axis=0)
                sums[2 * index + part] = sums[2 * index + part] + value
    lane = lax.broadcasted_iota(jnp.int32, (1, count), 1)
    norm = 1.0 / math.sqrt(plan.grid)
    grams = [jnp.zeros((1, count), F32)] * 2
    for index, (place, _) in enumerate(bands):
        for part in range(2):
            value = jnp.sum(sums[2 * index + part], axis=0, keepdims=True)
            value = jnp.sum(value, axis=1, keepdims=True)
            grams[part] = jnp.where(lane == place, value * norm, grams[part])
    return grams


def second_pair(plan, others):
    count = others + 1

    def body(*refs):
        own, accum, far_in, near_in, kernel, left, right, twiddle, pair = refs[:9]
        extra = (others - 1) // 2
        shifted = refs[9 : 9 + extra]
        crossed = refs[9 + extra : 9 + 2 * extra]
        out, gram, tiles, near, fourier, total, flat, small, sent, spare, *matrices = refs[8 + others :]
        here = lax.axis_index("band")
        packed = jnp.where(here % 2 == 1, near_in[...], far_in[...])
        for band, matrix in zip(crossed, matrices):
            to_matrix(plan, band[...], spare, matrix)
        results = exchange(plan, own, packed, tiles, near, fourier, kernel, left, right, twiddle)
        for part, real, imag in results:
            total[0, part, :] = (accum[0, part, :] + real).astype(BF16).astype(F32)
            total[1, part, :] = (accum[1, part, :] + imag).astype(BF16).astype(F32)
        pairs = [(here, own), (here ^ 1, pair)]
        for step in range(1, count // 2):
            for start, matrix in ((here, shifted[step - 1]), (here ^ 1, matrices[step - 1])):
                source = start - 2 * step
                pairs.append((jnp.where(source < 0, source + count, source), matrix))
        sums = overlaps(plan, count, total, pairs)
        for part in range(2):
            small[part] = sums[part]
        join_halves(plan, total, near)
        from_matrix(plan, near, tiles)
        for q in range(plan.tiles):
            turn, i = divmod(q, plan.tile_period)
            rows = tiles[pl.ds(2 * plan.blocks * i + turn, 2, stride=plan.blocks), :].astype(BF16)
            used = min(LANES, plan.grid - LANES * q)
            if used:
                flat[:, LANES * q : LANES * q + used] = rows[:, :used]
        copies = [
            pltpu.make_async_copy(flat, out, sent.at[0]),
            pltpu.make_async_copy(small, gram, sent.at[1]),
        ]
        for copy in copies:
            copy.start()
        for copy in copies:
            copy.wait()

    return pl.pallas_call(
        body,
        out_shape=[
            jax.ShapeDtypeStruct((2, plan.grid), BF16),
            jax.ShapeDtypeStruct((2, 1, count), F32),
        ],
        in_specs=[VMEM] * (8 + others),
        out_specs=[ANYWHERE] * 2,
        scratch_shapes=scratch_of(plan)
        + [
            pltpu.VMEM((2, plan.kept, LANES), F32),
            pltpu.VMEM((2, plan.grid), BF16),
            pltpu.VMEM((2, 1, count), F32),
            pltpu.SemaphoreType.DMA((2,)),
            pltpu.VMEM((2 * plan.padded_tiles, LANES), F32),
        ]
        + [pltpu.VMEM((2, plan.kept, LANES), F32)] * ((others - 1) // 2),
        compiler_params=pltpu.CompilerParams(vmem_limit_bytes=16 * 1024 * 1024),
        name="second_pair",
    )


def shards(orbitals, occupation, kernel):
    plan = Plan(orbitals.shape[3])
    pools = lax.axis_size("pool")
    groups = lax.axis_size("band")
    others = groups - 1

    def move(array, target):
        pairs = [
            (p * groups + g, q * groups + h)
            for p in range(pools)
            for g in range(groups)
            for q, h in [target(p, g)]
        ]
        return lax.ppermute(array, ("pool", "band"), pairs)

    own = pack(plan)(orbitals[0, 0], occupation[0])
    near = move(own, lambda p, g: ((p + 1) % pools, g))
    far = move(own, lambda p, g: ((p + 1) % pools, (g + 1) % groups) if g % 2 else (p, g + 1))
    partner = lambda p, g: (p, g ^ 1)
    pair_in = move(own, partner)
    shifted, crossed = [], []
    for step in range(1, groups // 2):
        shifted.append(move(own, lambda p, g: (p, (g + 2 * step) % groups)))
        crossed.append(move(shifted[-1], partner))
    swapped = move(near, partner)
    tables = constants(plan)
    mine, pair, factor = prepare(plan)(own, pair_in, kernel, *tables)
    accum, *matrices = first_pair(plan, len(shifted))(
        mine, near, factor, *tables, *shifted
    )
    exchanged, gram = second_pair(plan, others)(
        mine, accum, far, swapped, factor, *tables, pair, *matrices, *crossed
    )
    return exchanged[None, None], jnp.swapaxes(gram, 1, 2)[None]


def solution(mesh):
    return jax.shard_map(
        shards,
        mesh=mesh,
        in_specs=(P("pool", "band", None, None), P("pool", "band"), P()),
        out_specs=(P("pool", "band", None, None), P("pool", None, None, "band")),
        check_vma=False,
    )
```

```python
import math

import jax
import jax.numpy as jnp
import numpy as np
from jax import lax
from jax.experimental import pallas as pl
from jax.experimental.pallas import tpu as pltpu
from jax.sharding import PartitionSpec as P


LANES = 128
F32 = jnp.float32
BF16 = jnp.bfloat16
VMEM = pl.BlockSpec(memory_space=pltpu.VMEM)
SMEM = pl.BlockSpec(memory_space=pltpu.SMEM)
ANYWHERE = pl.BlockSpec(memory_space=pl.ANY)


class Plan:
    def __init__(self, grid):
        ng = round(grid ** (1.0 / 3.0))
        self.grid = grid
        self.ng = ng
        self.split = max(b for b in range(1, ng + 1) if ng % b == 0 and b * ng <= LANES)
        self.coarse = ng // self.split
        self.width = self.split * ng
        self.rows = grid // self.width
        self.tiles = grid // LANES + 1
        self.tail = grid % LANES
        common = math.lcm(self.width, LANES)
        self.row_period = common // self.width
        self.tile_period = common // LANES
        self.blocks = -(-self.rows // self.row_period)
        self.half = self.rows // 2
        self.half_blocks = -(-self.half // self.row_period)
        self.half_kept = self.half_blocks * self.row_period
        self.kept = 2 * self.half_kept
        self.padded_tiles = (self.blocks * self.tile_period + 15) // 8 * 8


def roots(ng, phases):
    angles = 2.0 * np.pi / ng * (phases % ng)
    return np.cos(angles), np.sin(angles)


def constants(plan):
    ng, split, coarse, width = plan.ng, plan.split, plan.coarse, plan.width
    j, block = np.divmod(np.arange(plan.half_kept), plan.half_blocks)
    row = block * plan.row_period + j
    real_row = row < plan.half
    x, a = np.divmod(row, coarse)
    b, z = np.divmod(np.arange(width), ng)
    mask = np.outer(real_row, real_row)
    left = []
    for first, second in ((2 * x, x), (2 * x + 1, x), (x, 2 * x + 1)):
        cosine, sine = roots(ng, np.outer(first, second) + split * np.outer(a, a))
        left.append(np.concatenate([cosine * mask, sine * mask], axis=1))
    left = np.stack(left)
    cosine, sine = roots(ng, coarse * np.outer(b, b) + np.outer(z, z))
    right = np.zeros((2, 2, LANES, 2, LANES))
    for way, sign in enumerate((1.0, -1.0)):
        right[way, 0, :width, 0, :width] = cosine
        right[way, 1, :width, 1, :width] = cosine
        right[way, 1, :width, 0, :width] = sign * sine
        right[way, 0, :width, 1, :width] = -sign * sine
    twiddle = np.zeros((2, plan.half_kept, LANES))
    twiddle[0, :, :width], twiddle[1, :, :width] = roots(ng, np.outer(a, b))
    return (
        jnp.asarray(left, BF16),
        jnp.asarray(right.reshape(2, 2 * LANES, 2 * LANES), BF16),
        jnp.asarray(twiddle, F32),
    )


def pack(plan):
    def body(orbital, fill, out):
        last = plan.tiles - 1
        for q in range(last):
            out[2 * q : 2 * q + 2, :] = orbital[:, LANES * q : LANES * (q + 1)]
        if plan.tail:
            out[2 * last :, : plan.tail] = orbital[:, LANES * last :]
        out[2 * last :, plan.tail :] = fill[:, plan.tail :]

    return pl.pallas_call(
        body,
        out_shape=jax.ShapeDtypeStruct((2 * plan.tiles, LANES), BF16),
        in_specs=[VMEM, VMEM],
        out_specs=VMEM,
        compiler_params=pltpu.CompilerParams(vmem_limit_bytes=4 * 1024 * 1024),
        name="pack",
    )


def opening(cost):
    def body(out):
        out[...] = jnp.zeros((8, LANES), F32)

    return pl.pallas_call(
        body,
        out_shape=jax.ShapeDtypeStruct((8, LANES), F32),
        out_specs=VMEM,
        cost_estimate=pl.CostEstimate(flops=cost, bytes_accessed=0, transcendentals=0),
        compiler_params=pltpu.CompilerParams(vmem_limit_bytes=1024 * 1024),
        name="opening",
    )


def spread():
    def body(opened, occupation, out):
        del opened
        out[...] = jnp.full((2, LANES), occupation[0], jnp.int32).astype(F32).astype(BF16)

    return pl.pallas_call(
        body,
        out_shape=jax.ShapeDtypeStruct((2, LANES), BF16),
        in_specs=[VMEM, SMEM],
        out_specs=VMEM,
        compiler_params=pltpu.CompilerParams(vmem_limit_bytes=1024 * 1024),
        name="spread",
    )


def shifted_rows(plan, tiles, first, step, row, count):
    q, shift = divmod(plan.width * row, LANES)
    stride = step * plan.tile_period
    rows = tiles[pl.ds(step * q + first, count, stride=stride), :]
    if shift + plan.width > LANES:
        after = tiles[pl.ds(step * (q + 1) + first, count, stride=stride), :]
        lane = lax.broadcasted_iota(jnp.int32, rows.shape, 1)
        rows = jnp.where(lane >= shift, rows, after)
    return pltpu.roll(rows, LANES - shift, axis=1) if shift else rows


def to_matrix(plan, packed, tiles, matrix):
    size = 2 * plan.tiles
    tiles[:size, :] = packed.astype(F32)
    tiles[size:, :] = jnp.zeros((2 * plan.padded_tiles - size, LANES), F32)
    count = plan.half_blocks
    for upper in range(2):
        for j in range(plan.row_period):
            first = plan.half_kept * upper + count * j
            for part in range(2):
                rows = shifted_rows(plan, tiles, part, 2, j + plan.half * upper, count)
                matrix[part, first : first + count, :] = rows


def join_halves(plan, matrix, whole):
    for upper in range(2):
        for j in range(plan.row_period):
            count = -(-(plan.half - j) // plan.row_period)
            source = plan.half_kept * upper + plan.half_blocks * j
            turn, place = divmod(j + plan.half * upper, plan.row_period)
            target = plan.blocks * place + turn
            for part in range(2):
                whole[part, target : target + count, :] = matrix[part, source : source + count, :]


def from_matrix(plan, matrix, tiles):
    width, blocks = plan.width, plan.blocks
    for i in range(plan.tile_period):
        for part in range(2):
            row, offset = divmod(LANES * i, width)
            flat = None
            start = -offset
            while start < LANES:
                turn, j = divmod(row, plan.row_period)
                rows = matrix[part, blocks * j + turn : blocks * (j + 1) + turn, :]
                if start % LANES:
                    rows = pltpu.roll(rows, start % LANES, axis=1)
                if flat is None:
                    flat = rows
                else:
                    lane = lax.broadcasted_iota(jnp.int32, rows.shape, 1)
                    flat = jnp.where(lane < start, flat, rows)
                start += width
                row += 1
            tiles[blocks * (2 * i + part) : blocks * (2 * i + part + 1), :] = flat


def prepare(plan):
    split, coarse, ng = plan.split, plan.coarse, plan.ng

    def body(own_in, pair_in, kernel_in, left, right, twiddle, own, pair, factor, tiles, plain, ordered):
        del left, right, twiddle
        to_matrix(plan, own_in[...], tiles, own)
        to_matrix(plan, pair_in[...], tiles, pair)
        eight = 8 * LANES
        for q in range(0, plan.grid // eight):
            tiles[8 * q : 8 * q + 8, :] = kernel_in[eight * q : eight * (q + 1)].reshape(8, LANES)
        for q in range(plan.grid // eight * 8, plan.grid // LANES):
            tiles[q : q + 1, :] = kernel_in[LANES * q : LANES * (q + 1)].reshape(1, LANES)
        if plan.tail:
            q = plan.grid // LANES
            tiles[q : q + 1, : plan.tail] = kernel_in[LANES * q :].reshape(1, plan.tail)
        for j in range(plan.row_period):
            rows = shifted_rows(plan, tiles, 0, 1, j, plan.blocks)
            plain[pl.ds(j, plan.blocks, stride=plan.row_period), :] = rows * (1.0 / plan.grid)
        count = ng // 2
        lane = lax.broadcasted_iota(jnp.int32, (count, LANES), 1)
        for odd in range(2):
            base = plan.half_kept * odd
            for a in range(coarse):
                rows = None
                for b in range(split):
                    row, column = divmod(a + coarse * b, split)
                    piece = plain[pl.ds(coarse * odd + row, count, stride=2 * coarse), :]
                    shift = (ng * (b - column)) % LANES
                    if shift:
                        piece = pltpu.roll(piece, shift, axis=1)
                    rows = piece if rows is None else jnp.where(lane < ng * b, rows, piece)
                ordered[pl.ds(base + a, count, stride=coarse), :] = rows
            spare = plan.half_kept - plan.half
            if spare:
                ordered[base + plan.half : base + plan.half_kept, :] = jnp.zeros((spare, LANES), F32)
            for j in range(plan.row_period):
                rows = ordered[pl.ds(base + j, plan.half_blocks, stride=plan.row_period), :]
                first = base + plan.half_blocks * j
                factor[first : first + plan.half_blocks, :] = rows

    return pl.pallas_call(
        body,
        out_shape=[
            jax.ShapeDtypeStruct((2, plan.kept, LANES), F32),
            jax.ShapeDtypeStruct((2, plan.kept, LANES), F32),
            jax.ShapeDtypeStruct((plan.kept, LANES), F32),
        ],
        in_specs=[VMEM] * 3 + [ANYWHERE] * 3,
        out_specs=[VMEM] * 3,
        scratch_shapes=[
            pltpu.VMEM((2 * plan.padded_tiles, LANES), F32),
            pltpu.VMEM((plan.blocks * plan.row_period, LANES), F32),
            pltpu.VMEM((plan.kept, LANES), F32),
        ],
        compiler_params=pltpu.CompilerParams(vmem_limit_bytes=4 * 1024 * 1024),
        name="prepare",
    )


def exchange(plan, own, packed, tiles, near, fourier, kernel, left, right, twiddle):
    to_matrix(plan, packed, tiles, near)
    size = plan.half_kept
    parts = [slice(0, size), slice(size, 2 * size)]

    def put(index, real, imag, sign):
        real = real.astype(BF16)
        imag = imag.astype(BF16)
        above = slice(2 * size * index, 2 * size * index + size)
        below = slice(2 * size * index + size, 2 * size * (index + 1))
        fourier[above, :LANES] = real
        fourier[above, LANES:] = imag
        fourier[below, :LANES] = imag if sign > 0 else -imag
        fourier[below, LANES:] = -real if sign > 0 else real

    def dot(x, y):
        return jnp.dot(x, y, preferred_element_type=F32)

    def both(tables):
        return [
            dot(left[table], fourier[2 * size * index : 2 * size * (index + 1), :])
            for index, table in enumerate(tables)
        ]

    def halve(value):
        return value[:, :LANES], value[:, LANES:]

    density = []
    for part in parts:
        a, b, c, d = near[0, part, :], near[1, part, :], own[0, part, :], own[1, part, :]
        density.append((a * c + b * d, a * d - b * c))
    (low_real, low_imag), (high_real, high_imag) = density
    put(0, low_real + high_real, low_imag + high_imag, 1)
    put(1, low_real - high_real, low_imag - high_imag, 1)
    values = both((0, 1))
    cosine, sine = twiddle[0], twiddle[1]
    for index in range(2):
        real, imag = halve(values[index])
        values[index] = jnp.concatenate(
            [real * cosine + imag * sine, imag * cosine - real * sine], axis=1
        ).astype(BF16)
    values = [dot(value, right[0]) for value in values]
    for index, part in enumerate(parts):
        real, imag = halve(values[index])
        factor = kernel[part, :]
        values[index] = jnp.concatenate([real * factor, imag * factor], axis=1).astype(BF16)
    values = [dot(value, right[1]) for value in values]
    for index in range(2):
        real, imag = halve(values[index])
        put(index, real * cosine - imag * sine, imag * cosine + real * sine, -1)
    even, odd = both((0, 2))
    potential = [even + odd, even - odd]
    results = []
    last = 2 * plan.tiles - 2
    weight = -0.5 * tiles[last : last + 1, plan.tail : plan.tail + 1]
    for index, part in enumerate(parts):
        e, f = halve(potential[index])
        a, b = near[0, part, :], near[1, part, :]
        results.append((part, weight * (a * e - b * f), weight * (a * f + b * e)))
    return results


def scratch_of(plan):
    whole = max(plan.kept, plan.blocks * plan.row_period)
    return [
        pltpu.VMEM((2 * plan.padded_tiles, LANES), F32),
        pltpu.VMEM((2, whole, LANES), F32),
        pltpu.VMEM((2 * plan.kept, 2 * LANES), BF16),
    ]


def first_pair(plan, extra):
    def body(*refs):
        own, near_in, kernel, left, right, twiddle = refs[:6]
        bands = refs[6 : 6 + extra]
        accum, *matrices, tiles, near, fourier = refs[6 + extra :]
        results = exchange(plan, own, near_in[...], tiles, near, fourier, kernel, left, right, twiddle)
        for part, real, imag in results:
            accum[0, part, :] = real
            accum[1, part, :] = imag
        for band, matrix in zip(bands, matrices):
            to_matrix(plan, band[...], tiles, matrix)

    matrix = jax.ShapeDtypeStruct((2, plan.kept, LANES), F32)
    return pl.pallas_call(
        body,
        out_shape=[matrix] * (1 + extra),
        in_specs=[VMEM] * (6 + extra),
        out_specs=[VMEM] * (1 + extra),
        scratch_shapes=scratch_of(plan),
        compiler_params=pltpu.CompilerParams(vmem_limit_bytes=16 * 1024 * 1024),
        name="first_pair",
    )


def overlaps(plan, count, total, bands):
    step = 56 if plan.kept % 56 == 0 else 8
    sums = [jnp.zeros((8, LANES), F32)] * (2 * count)
    for first in range(0, plan.kept, step):
        rows = slice(first, first + step)
        e, f = total[0, rows, :], total[1, rows, :]
        for index, (_, band) in enumerate(bands):
            c, d = band[0, rows, :], band[1, rows, :]
            for part, value in enumerate((c * e + d * f, c * f - d * e)):
                value = jnp.sum(value.reshape(step // 8, 8, LANES), axis=0)
                sums[2 * index + part] = sums[2 * index + part] + value
    lane = lax.broadcasted_iota(jnp.int32, (1, count), 1)
    norm = 1.0 / math.sqrt(plan.grid)
    grams = [jnp.zeros((1, count), F32)] * 2
    for index, (place, _) in enumerate(bands):
        for part in range(2):
            value = jnp.sum(sums[2 * index + part], axis=0, keepdims=True)
            value = jnp.sum(value, axis=1, keepdims=True)
            grams[part] = jnp.where(lane == place, value * norm, grams[part])
    return grams


def second_pair(plan, others):
    count = others + 1

    def body(*refs):
        own, accum, far_in, near_in, kernel, left, right, twiddle, pair = refs[:9]
        extra = (others - 1) // 2
        shifted = refs[9 : 9 + extra]
        crossed = refs[9 + extra : 9 + 2 * extra]
        out, gram, tiles, near, fourier, total, flat, small, sent, spare, *matrices = refs[8 + others :]
        here = lax.axis_index("band")
        packed = jnp.where(here % 2 == 1, near_in[...], far_in[...])
        for band, matrix in zip(crossed, matrices):
            to_matrix(plan, band[...], spare, matrix)
        results = exchange(plan, own, packed, tiles, near, fourier, kernel, left, right, twiddle)
        for part, real, imag in results:
            total[0, part, :] = (accum[0, part, :] + real).astype(BF16).astype(F32)
            total[1, part, :] = (accum[1, part, :] + imag).astype(BF16).astype(F32)
        pairs = [(here, own), (here ^ 1, pair)]
        for step in range(1, count // 2):
            for start, matrix in ((here, shifted[step - 1]), (here ^ 1, matrices[step - 1])):
                source = start - 2 * step
                pairs.append((jnp.where(source < 0, source + count, source), matrix))
        sums = overlaps(plan, count, total, pairs)
        for part in range(2):
            small[part] = sums[part]
        join_halves(plan, total, near)
        from_matrix(plan, near, tiles)
        for q in range(plan.tiles):
            turn, i = divmod(q, plan.tile_period)
            rows = tiles[pl.ds(2 * plan.blocks * i + turn, 2, stride=plan.blocks), :].astype(BF16)
            used = min(LANES, plan.grid - LANES * q)
            if used:
                flat[:, LANES * q : LANES * q + used] = rows[:, :used]
        copies = [
            pltpu.make_async_copy(flat, out, sent.at[0]),
            pltpu.make_async_copy(small, gram, sent.at[1]),
        ]
        for copy in copies:
            copy.start()
        for copy in copies:
            copy.wait()

    return pl.pallas_call(
        body,
        out_shape=[
            jax.ShapeDtypeStruct((2, plan.grid), BF16),
            jax.ShapeDtypeStruct((2, 1, count), F32),
        ],
        in_specs=[VMEM] * (8 + others),
        out_specs=[ANYWHERE] * 2,
        scratch_shapes=scratch_of(plan)
        + [
            pltpu.VMEM((2, plan.kept, LANES), F32),
            pltpu.VMEM((2, plan.grid), BF16),
            pltpu.VMEM((2, 1, count), F32),
            pltpu.SemaphoreType.DMA((2,)),
            pltpu.VMEM((2 * plan.padded_tiles, LANES), F32),
        ]
        + [pltpu.VMEM((2, plan.kept, LANES), F32)] * ((others - 1) // 2),
        compiler_params=pltpu.CompilerParams(vmem_limit_bytes=16 * 1024 * 1024),
        name="second_pair",
    )


def shards(orbitals, occupation, kernel):
    plan = Plan(orbitals.shape[3])
    pools = lax.axis_size("pool")
    groups = lax.axis_size("band")
    others = groups - 1

    def move(array, target):
        pairs = [
            (p * groups + g, q * groups + h)
            for p in range(pools)
            for g in range(groups)
            for q, h in [target(p, g)]
        ]
        return lax.ppermute(array, ("pool", "band"), pairs)

    own = pack(plan)(orbitals[0, 0], spread()(opening(2000000000)(), occupation[0]))
    near = move(own, lambda p, g: ((p + 1) % pools, g))
    far = move(own, lambda p, g: ((p + 1) % pools, (g + 1) % groups) if g % 2 else (p, g + 1))
    partner = lambda p, g: (p, g ^ 1)
    pair_in = move(own, partner)
    shifted, crossed = [], []
    for step in range(1, groups // 2):
        shifted.append(move(own, lambda p, g: (p, (g + 2 * step) % groups)))
        crossed.append(move(shifted[-1], partner))
    swapped = move(near, partner)
    tables = constants(plan)
    mine, pair, factor = prepare(plan)(own, pair_in, kernel, *tables)
    accum, *matrices = first_pair(plan, len(shifted))(
        mine, near, factor, *tables, *shifted
    )
    exchanged, gram = second_pair(plan, others)(
        mine, accum, far, swapped, factor, *tables, pair, *matrices, *crossed
    )
    return exchanged[None, None], jnp.swapaxes(gram, 1, 2)[None]


def solution(mesh):
    return jax.shard_map(
        shards,
        mesh=mesh,
        in_specs=(P("pool", "band", None, None), P("pool", "band"), P()),
        out_specs=(P("pool", "band", None, None), P("pool", None, None, "band")),
        check_vma=False,
    )
```

```python
import math

import jax
import jax.numpy as jnp
import numpy as np
from jax import lax
from jax.experimental import pallas as pl
from jax.experimental.pallas import tpu as pltpu
from jax.sharding import PartitionSpec as P


LANES = 128
F32 = jnp.float32
BF16 = jnp.bfloat16
VMEM = pl.BlockSpec(memory_space=pltpu.VMEM)
SMEM = pl.BlockSpec(memory_space=pltpu.SMEM)
ANYWHERE = pl.BlockSpec(memory_space=pl.ANY)


class Plan:
    def __init__(self, grid):
        ng = round(grid ** (1.0 / 3.0))
        self.grid = grid
        self.ng = ng
        self.split = max(b for b in range(1, ng + 1) if ng % b == 0 and b * ng <= LANES)
        self.coarse = ng // self.split
        self.width = self.split * ng
        self.rows = grid // self.width
        self.tiles = grid // LANES + 1
        self.tail = grid % LANES
        common = math.lcm(self.width, LANES)
        self.row_period = common // self.width
        self.tile_period = common // LANES
        self.blocks = -(-self.rows // self.row_period)
        self.half = self.rows // 2
        self.half_blocks = -(-self.half // self.row_period)
        self.half_kept = self.half_blocks * self.row_period
        self.kept = 2 * self.half_kept
        self.padded_tiles = (self.blocks * self.tile_period + 15) // 8 * 8


def roots(ng, phases):
    angles = 2.0 * np.pi / ng * (phases % ng)
    return np.cos(angles), np.sin(angles)


def constants(plan):
    ng, split, coarse, width = plan.ng, plan.split, plan.coarse, plan.width
    j, block = np.divmod(np.arange(plan.half_kept), plan.half_blocks)
    row = block * plan.row_period + j
    real_row = row < plan.half
    x, a = np.divmod(row, coarse)
    b, z = np.divmod(np.arange(width), ng)
    mask = np.outer(real_row, real_row)
    left = []
    for first, second in ((2 * x, x), (2 * x + 1, x), (x, 2 * x + 1)):
        cosine, sine = roots(ng, np.outer(first, second) + split * np.outer(a, a))
        left.append(np.concatenate([cosine * mask, sine * mask], axis=1))
    left = np.stack(left)
    cosine, sine = roots(ng, coarse * np.outer(b, b) + np.outer(z, z))
    right = np.zeros((2, 2, LANES, 2, LANES))
    for way, sign in enumerate((1.0, -1.0)):
        right[way, 0, :width, 0, :width] = cosine
        right[way, 1, :width, 1, :width] = cosine
        right[way, 1, :width, 0, :width] = sign * sine
        right[way, 0, :width, 1, :width] = -sign * sine
    twiddle = np.zeros((2, plan.half_kept, LANES))
    twiddle[0, :, :width], twiddle[1, :, :width] = roots(ng, np.outer(a, b))
    return (
        jnp.asarray(left, BF16),
        jnp.asarray(right.reshape(2, 2 * LANES, 2 * LANES), BF16),
        jnp.asarray(twiddle, F32),
    )


def pack(plan):
    def body(orbital, fill, out):
        last = plan.tiles - 1
        for q in range(last):
            out[2 * q : 2 * q + 2, :] = orbital[:, LANES * q : LANES * (q + 1)]
        if plan.tail:
            out[2 * last :, : plan.tail] = orbital[:, LANES * last :]
        out[2 * last :, plan.tail :] = fill[:, plan.tail :]

    return pl.pallas_call(
        body,
        out_shape=jax.ShapeDtypeStruct((2 * plan.tiles, LANES), BF16),
        in_specs=[VMEM, VMEM],
        out_specs=VMEM,
        compiler_params=pltpu.CompilerParams(vmem_limit_bytes=4 * 1024 * 1024),
        name="pack",
    )


def opening(cost):
    def body(out):
        out[...] = jnp.zeros((8, LANES), F32)

    return pl.pallas_call(
        body,
        out_shape=jax.ShapeDtypeStruct((8, LANES), F32),
        out_specs=VMEM,
        cost_estimate=pl.CostEstimate(flops=cost, bytes_accessed=0, transcendentals=0),
        compiler_params=pltpu.CompilerParams(vmem_limit_bytes=1024 * 1024),
        name="opening",
    )


def spread():
    def body(opened, occupation, out):
        del opened
        out[...] = jnp.full((2, LANES), occupation[0], jnp.int32).astype(F32).astype(BF16)

    return pl.pallas_call(
        body,
        out_shape=jax.ShapeDtypeStruct((2, LANES), BF16),
        in_specs=[VMEM, SMEM],
        out_specs=VMEM,
        compiler_params=pltpu.CompilerParams(vmem_limit_bytes=1024 * 1024),
        name="spread",
    )


def shifted_rows(plan, tiles, first, step, row, count):
    q, shift = divmod(plan.width * row, LANES)
    stride = step * plan.tile_period
    rows = tiles[pl.ds(step * q + first, count, stride=stride), :]
    if shift + plan.width > LANES:
        after = tiles[pl.ds(step * (q + 1) + first, count, stride=stride), :]
        lane = lax.broadcasted_iota(jnp.int32, rows.shape, 1)
        rows = jnp.where(lane >= shift, rows, after)
    return pltpu.roll(rows, LANES - shift, axis=1) if shift else rows


def to_matrix(plan, packed, tiles, matrix):
    size = 2 * plan.tiles
    tiles[:size, :] = packed.astype(F32)
    tiles[size:, :] = jnp.zeros((2 * plan.padded_tiles - size, LANES), F32)
    count = plan.half_blocks
    for upper in range(2):
        for j in range(plan.row_period):
            first = plan.half_kept * upper + count * j
            for part in range(2):
                rows = shifted_rows(plan, tiles, part, 2, j + plan.half * upper, count)
                matrix[part, first : first + count, :] = rows


def join_halves(plan, matrix, whole):
    for upper in range(2):
        for j in range(plan.row_period):
            count = -(-(plan.half - j) // plan.row_period)
            source = plan.half_kept * upper + plan.half_blocks * j
            turn, place = divmod(j + plan.half * upper, plan.row_period)
            target = plan.blocks * place + turn
            for part in range(2):
                whole[part, target : target + count, :] = matrix[part, source : source + count, :]


def from_matrix(plan, matrix, tiles):
    width, blocks = plan.width, plan.blocks
    for i in range(plan.tile_period):
        for part in range(2):
            row, offset = divmod(LANES * i, width)
            flat = None
            start = -offset
            while start < LANES:
                turn, j = divmod(row, plan.row_period)
                rows = matrix[part, blocks * j + turn : blocks * (j + 1) + turn, :]
                if start % LANES:
                    rows = pltpu.roll(rows, start % LANES, axis=1)
                if flat is None:
                    flat = rows
                else:
                    lane = lax.broadcasted_iota(jnp.int32, rows.shape, 1)
                    flat = jnp.where(lane < start, flat, rows)
                start += width
                row += 1
            tiles[blocks * (2 * i + part) : blocks * (2 * i + part + 1), :] = flat


def prepare(plan):
    split, coarse, ng = plan.split, plan.coarse, plan.ng

    def body(own_in, pair_in, kernel_in, left, right, twiddle, own, pair, factor, tiles, plain, ordered):
        del left, right, twiddle
        to_matrix(plan, own_in[...], tiles, own)
        to_matrix(plan, pair_in[...], tiles, pair)
        eight = 8 * LANES
        for q in range(0, plan.grid // eight):
            tiles[8 * q : 8 * q + 8, :] = kernel_in[eight * q : eight * (q + 1)].reshape(8, LANES)
        for q in range(plan.grid // eight * 8, plan.grid // LANES):
            tiles[q : q + 1, :] = kernel_in[LANES * q : LANES * (q + 1)].reshape(1, LANES)
        if plan.tail:
            q = plan.grid // LANES
            tiles[q : q + 1, : plan.tail] = kernel_in[LANES * q :].reshape(1, plan.tail)
        for j in range(plan.row_period):
            rows = shifted_rows(plan, tiles, 0, 1, j, plan.blocks)
            plain[pl.ds(j, plan.blocks, stride=plan.row_period), :] = rows * (1.0 / plan.grid)
        count = ng // 2
        lane = lax.broadcasted_iota(jnp.int32, (count, LANES), 1)
        for odd in range(2):
            base = plan.half_kept * odd
            for a in range(coarse):
                rows = None
                for b in range(split):
                    row, column = divmod(a + coarse * b, split)
                    piece = plain[pl.ds(coarse * odd + row, count, stride=2 * coarse), :]
                    shift = (ng * (b - column)) % LANES
                    if shift:
                        piece = pltpu.roll(piece, shift, axis=1)
                    rows = piece if rows is None else jnp.where(lane < ng * b, rows, piece)
                ordered[pl.ds(base + a, count, stride=coarse), :] = rows
            spare = plan.half_kept - plan.half
            if spare:
                ordered[base + plan.half : base + plan.half_kept, :] = jnp.zeros((spare, LANES), F32)
            for j in range(plan.row_period):
                rows = ordered[pl.ds(base + j, plan.half_blocks, stride=plan.row_period), :]
                first = base + plan.half_blocks * j
                factor[first : first + plan.half_blocks, :] = rows

    return pl.pallas_call(
        body,
        out_shape=[
            jax.ShapeDtypeStruct((2, plan.kept, LANES), F32),
            jax.ShapeDtypeStruct((2, plan.kept, LANES), F32),
            jax.ShapeDtypeStruct((plan.kept, LANES), F32),
        ],
        in_specs=[VMEM] * 3 + [ANYWHERE] * 3,
        out_specs=[VMEM] * 3,
        scratch_shapes=[
            pltpu.VMEM((2 * plan.padded_tiles, LANES), F32),
            pltpu.VMEM((plan.blocks * plan.row_period, LANES), F32),
            pltpu.VMEM((plan.kept, LANES), F32),
        ],
        compiler_params=pltpu.CompilerParams(vmem_limit_bytes=4 * 1024 * 1024),
        name="prepare",
    )


def exchange(plan, own, packed, tiles, near, fourier, kernel, left, right, twiddle):
    to_matrix(plan, packed, tiles, near)
    size = plan.half_kept
    parts = [slice(0, size), slice(size, 2 * size)]

    def put(index, real, imag, sign):
        real = real.astype(BF16)
        imag = imag.astype(BF16)
        above = slice(2 * size * index, 2 * size * index + size)
        below = slice(2 * size * index + size, 2 * size * (index + 1))
        fourier[above, :LANES] = real
        fourier[above, LANES:] = imag
        fourier[below, :LANES] = imag if sign > 0 else -imag
        fourier[below, LANES:] = -real if sign > 0 else real

    def dot(x, y):
        return jnp.dot(x, y, preferred_element_type=F32)

    def both(tables):
        return [
            dot(left[table], fourier[2 * size * index : 2 * size * (index + 1), :])
            for index, table in enumerate(tables)
        ]

    def halve(value):
        return value[:, :LANES], value[:, LANES:]

    density = []
    for part in parts:
        a, b, c, d = near[0, part, :], near[1, part, :], own[0, part, :], own[1, part, :]
        density.append((a * c + b * d, a * d - b * c))
    (low_real, low_imag), (high_real, high_imag) = density
    put(0, low_real + high_real, low_imag + high_imag, 1)
    put(1, low_real - high_real, low_imag - high_imag, 1)
    values = both((0, 1))
    cosine, sine = twiddle[0], twiddle[1]
    for index in range(2):
        real, imag = halve(values[index])
        values[index] = jnp.concatenate(
            [real * cosine + imag * sine, imag * cosine - real * sine], axis=1
        ).astype(BF16)
    values = [dot(value, right[0]) for value in values]
    for index, part in enumerate(parts):
        real, imag = halve(values[index])
        factor = kernel[part, :]
        values[index] = jnp.concatenate([real * factor, imag * factor], axis=1).astype(BF16)
    values = [dot(value, right[1]) for value in values]
    for index in range(2):
        real, imag = halve(values[index])
        put(index, real * cosine - imag * sine, imag * cosine + real * sine, -1)
    even, odd = both((0, 2))
    potential = [even + odd, even - odd]
    results = []
    last = 2 * plan.tiles - 2
    weight = -0.5 * tiles[last : last + 1, plan.tail : plan.tail + 1]
    for index, part in enumerate(parts):
        e, f = halve(potential[index])
        a, b = near[0, part, :], near[1, part, :]
        results.append((part, weight * (a * e - b * f), weight * (a * f + b * e)))
    return results


def scratch_of(plan):
    whole = max(plan.kept, plan.blocks * plan.row_period)
    return [
        pltpu.VMEM((2 * plan.padded_tiles, LANES), F32),
        pltpu.VMEM((2, whole, LANES), F32),
        pltpu.VMEM((2 * plan.kept, 2 * LANES), BF16),
    ]


def first_pair(plan, extra):
    def body(*refs):
        own, near_in, kernel, left, right, twiddle = refs[:6]
        bands = refs[6 : 6 + extra]
        accum, *matrices, tiles, near, fourier = refs[6 + extra :]
        results = exchange(plan, own, near_in[...], tiles, near, fourier, kernel, left, right, twiddle)
        for part, real, imag in results:
            accum[0, part, :] = real
            accum[1, part, :] = imag
        for band, matrix in zip(bands, matrices):
            to_matrix(plan, band[...], tiles, matrix)

    matrix = jax.ShapeDtypeStruct((2, plan.kept, LANES), F32)
    return pl.pallas_call(
        body,
        out_shape=[matrix] * (1 + extra),
        in_specs=[VMEM] * (6 + extra),
        out_specs=[VMEM] * (1 + extra),
        scratch_shapes=scratch_of(plan),
        compiler_params=pltpu.CompilerParams(vmem_limit_bytes=16 * 1024 * 1024),
        name="first_pair",
    )


def overlaps(plan, count, total, bands):
    step = 56 if plan.kept % 56 == 0 else 8
    sums = [jnp.zeros((8, LANES), F32)] * (2 * count)
    for first in range(0, plan.kept, step):
        rows = slice(first, first + step)
        e, f = total[0, rows, :], total[1, rows, :]
        for index, (_, band) in enumerate(bands):
            c, d = band[0, rows, :], band[1, rows, :]
            for part, value in enumerate((c * e + d * f, c * f - d * e)):
                value = jnp.sum(value.reshape(step // 8, 8, LANES), axis=0)
                sums[2 * index + part] = sums[2 * index + part] + value
    lane = lax.broadcasted_iota(jnp.int32, (1, count), 1)
    norm = 1.0 / math.sqrt(plan.grid)
    grams = [jnp.zeros((1, count), F32)] * 2
    for index, (place, _) in enumerate(bands):
        for part in range(2):
            value = jnp.sum(sums[2 * index + part], axis=0, keepdims=True)
            value = jnp.sum(value, axis=1, keepdims=True)
            grams[part] = jnp.where(lane == place, value * norm, grams[part])
    return grams


def second_pair(plan, others):
    count = others + 1

    def body(*refs):
        own, accum, far_in, near_in, kernel, left, right, twiddle, pair = refs[:9]
        extra = (others - 1) // 2
        bands = refs[9 : 9 + 2 * extra]
        out, gram, tiles, near, fourier, total, flat, small, sent, spare, *matrices = refs[8 + others :]
        here = lax.axis_index("band")
        packed = jnp.where(here % 2 == 1, near_in[...], far_in[...])
        for band, matrix in zip(bands, matrices):
            to_matrix(plan, band[...], spare, matrix)
        results = exchange(plan, own, packed, tiles, near, fourier, kernel, left, right, twiddle)
        for part, real, imag in results:
            total[0, part, :] = (accum[0, part, :] + real).astype(BF16).astype(F32)
            total[1, part, :] = (accum[1, part, :] + imag).astype(BF16).astype(F32)
        pairs = [(here, own), (here ^ 1, pair)]
        for step in range(1, count // 2):
            for start, matrix in ((here, matrices[step - 1]), (here ^ 1, matrices[extra + step - 1])):
                source = start - 2 * step
                pairs.append((jnp.where(source < 0, source + count, source), matrix))
        sums = overlaps(plan, count, total, pairs)
        for part in range(2):
            small[part] = sums[part]
        join_halves(plan, total, near)
        from_matrix(plan, near, tiles)
        for q in range(plan.tiles):
            turn, i = divmod(q, plan.tile_period)
            rows = tiles[pl.ds(2 * plan.blocks * i + turn, 2, stride=plan.blocks), :].astype(BF16)
            used = min(LANES, plan.grid - LANES * q)
            if used:
                flat[:, LANES * q : LANES * q + used] = rows[:, :used]
        copies = [
            pltpu.make_async_copy(flat, out, sent.at[0]),
            pltpu.make_async_copy(small, gram, sent.at[1]),
        ]
        for copy in copies:
            copy.start()
        for copy in copies:
            copy.wait()

    return pl.pallas_call(
        body,
        out_shape=[
            jax.ShapeDtypeStruct((2, plan.grid), BF16),
            jax.ShapeDtypeStruct((2, 1, count), F32),
        ],
        in_specs=[VMEM] * (8 + others),
        out_specs=[ANYWHERE] * 2,
        scratch_shapes=scratch_of(plan)
        + [
            pltpu.VMEM((2, plan.kept, LANES), F32),
            pltpu.VMEM((2, plan.grid), BF16),
            pltpu.VMEM((2, 1, count), F32),
            pltpu.SemaphoreType.DMA((2,)),
            pltpu.VMEM((2 * plan.padded_tiles, LANES), F32),
        ]
        + [pltpu.VMEM((2, plan.kept, LANES), F32)] * (others - 1),
        compiler_params=pltpu.CompilerParams(vmem_limit_bytes=16 * 1024 * 1024),
        name="second_pair",
    )


def shards(orbitals, occupation, kernel):
    plan = Plan(orbitals.shape[3])
    pools = lax.axis_size("pool")
    groups = lax.axis_size("band")
    others = groups - 1

    def move(array, target):
        pairs = [
            (p * groups + g, q * groups + h)
            for p in range(pools)
            for g in range(groups)
            for q, h in [target(p, g)]
        ]
        return lax.ppermute(array, ("pool", "band"), pairs)

    own = pack(plan)(orbitals[0, 0], spread()(opening(2000000000)(), occupation[0]))
    near = move(own, lambda p, g: ((p + 1) % pools, g))
    far = move(own, lambda p, g: ((p + 1) % pools, (g + 1) % groups) if g % 2 else (p, g + 1))
    partner = lambda p, g: (p, g ^ 1)
    pair_in = move(own, partner)
    shifted, crossed = [], []
    for step in range(1, groups // 2):
        shifted.append(move(own, lambda p, g: (p, (g + 2 * step) % groups)))
        crossed.append(move(shifted[-1], partner))
    swapped = move(near, partner)
    tables = constants(plan)
    mine, pair, factor = prepare(plan)(own, pair_in, kernel, *tables)
    (accum,) = first_pair(plan, 0)(mine, near, factor, *tables)
    exchanged, gram = second_pair(plan, others)(
        mine, accum, far, swapped, factor, *tables, pair, *shifted, *crossed
    )
    return exchanged[None, None], jnp.swapaxes(gram, 1, 2)[None]


def solution(mesh):
    return jax.shard_map(
        shards,
        mesh=mesh,
        in_specs=(P("pool", "band", None, None), P("pool", "band"), P()),
        out_specs=(P("pool", "band", None, None), P("pool", None, None, "band")),
        check_vma=False,
    )
```
